256 devices in a mesh: wrow: 4 (over y), wcol: 16 (over z_hi, x), dom: 4 (over z_lo, core).
Axes of the slice: x: 4, y: 4, z: 8 (z_hi: 4, z_lo: 2; z = z_hi * 2 + z_lo), core: 2. Of those that a mesh axis runs over, the one named last changes fastest.
Arguments:
- positions: float32 [4, 16, 3, 8192], P('wrow', 'wcol', None, 'dom'), may hold values from -6 to 6
- velocities: float32 [4, 16, 3, 8192], P('wrow', 'wcol', None, 'dom'), may hold values from -6 to 6
- inv_mass: float32 [8192], P('dom'), may hold values from 0.5 to 2
- cv_weight: float32 [2, 3, 8192], P(None, None, 'dom'), may hold values from -0.125 to 0.125
- stiffness: float32 [2], replicated, may hold values from 1 to 4
- centers: float32 [4, 16, 2], P('wrow', 'wcol'), may hold values from -3 to 3
- block_order: int32 [8192], P('dom'), may hold values from 0 to 2047, as said below
- pair_count: int32 [4], P('dom'), may hold values from 16 to 64, as said below
- pair_own: int32 [4, 64], P('dom'), may hold values from 0 to 15, as said below
- pair_other: int32 [4, 64], P('dom'), may hold values from 0 to 47, as said below
- accept_row: int32 [4, 16], P('wrow', 'wcol'), may hold values from 0 to 1, as said below
- accept_col: int32 [4, 16], P('wrow', 'wcol'), may hold values from 0 to 1, as said below
Outputs:
- new_positions: float32 [4, 16, 3, 8192], P('wrow', 'wcol', None, 'dom')
- new_velocities: float32 [4, 16, 3, 8192], P('wrow', 'wcol', None, 'dom')
- new_forces: float32 [4, 16, 3, 8192], P('wrow', 'wcol', None, 'dom')
The draws below stay inside these ranges and needn't reach their ends.
Inputs may be any that keep to these rules, and one draw needn't show every extreme that they name: accept_row is equal for windows (2k, c) and (2k + 1, c). accept_col is equal for windows (r, 2k) and (r, 2k + 1). `block_order`: each slab's 2048 entries are a permutation of 0 to 2047. `pair_count`: some slab has exactly 64 live pairs. `pair_own`: entries past the slab's pair_count are 0. `pair_other`: slab 0 names no lower slab and the last slab no upper slab; entries past the slab's pair_count are 16.
All inputs are finite; a program needn't handle non-finite values.
Results may differ from the reference program's by a relative error of at most 0.0003.
Values sent between devices are 32-bit elements; how exact they have to be, the bound alone decides.
A program may use at most 64 MiB of HBM per device.

```python
import math
import jax
import jax.numpy as jnp
from jax import lax

ATOM_DEV = 2048
BLK = 128
STEPS = 3
NB = 16
PMAX = 64
ATOMS = 8192
NROW = 4
NCOL = 16


def counts_of(key):
    domains = ATOMS // ATOM_DEV
    base = jax.random.randint(jax.random.fold_in(key, 11), (domains,), PMAX // 4, PMAX + 1)
    chosen = jax.random.randint(jax.random.fold_in(key, 12), (), 0, domains)
    return jnp.where(jnp.arange(domains) == chosen, PMAX, base).astype(jnp.int32)


def live_slots(key):
    return jnp.arange(PMAX)[None, :] < counts_of(key)[:, None]


def draw_pair_count(key, part):
    return counts_of(key)


def draw_pair_own(key, part):
    domains = ATOMS // ATOM_DEV
    raw_blocks = jax.random.randint(jax.random.fold_in(key, 13), (domains, PMAX), 0, NB)
    return jnp.where(live_slots(key), raw_blocks, 0).astype(jnp.int32)


def draw_pair_other(key, part):
    domains = ATOMS // ATOM_DEV
    raw_blocks = jax.random.randint(jax.random.fold_in(key, 14), (domains, PMAX), 0, 3 * NB)
    slab_ids = jnp.arange(domains)[:, None]
    raw_blocks = jnp.where((slab_ids == 0) & (raw_blocks < NB), raw_blocks + NB, raw_blocks)
    raw_blocks = jnp.where((slab_ids == domains - 1) & (raw_blocks >= 2 * NB), raw_blocks - NB, raw_blocks)
    return jnp.where(live_slots(key), raw_blocks, NB).astype(jnp.int32)


def draw_block_order(key, part):
    domains = ATOMS // ATOM_DEV

    def one_slab(slab):
        return jax.random.permutation(jax.random.fold_in(key, 31 + slab), ATOM_DEV)
    return jax.vmap(one_slab)(jnp.arange(domains)).reshape(ATOMS).astype(jnp.int32)


def draw_accept_row(key, part):
    halves = jax.random.randint(jax.random.fold_in(key, 21), (NROW // 2, NCOL), 0, 2)
    halves = halves.at[0, 0].set(1).at[0, 1].set(0)
    return jnp.repeat(halves, 2, axis=0).astype(jnp.int32)


def draw_accept_col(key, part):
    halves = jax.random.randint(jax.random.fold_in(key, 22), (NROW, NCOL // 2), 0, 2)
    halves = halves.at[0, 0].set(1).at[1, 0].set(0)
    return jnp.repeat(halves, 2, axis=1).astype(jnp.int32)


def steps_of(stream_key, dims, cuts, smallest, largest):
    loudness = 1.0
    for axis_at, shards_of in cuts:
        heights = jax.random.uniform(jax.random.fold_in(jax.random.fold_in(stream_key, 6), axis_at), (shards_of,), jnp.float32, smallest / len(cuts), largest / len(cuts))
        loudness = loudness * jnp.repeat(jnp.exp(heights), dims[axis_at] // shards_of).reshape((-1,) + (1,) * (len(dims) - 1 - axis_at))
    return loudness


def scatter_about(key, extent, width, most, split=(), held_as=jnp.bfloat16):
    array = width * jax.random.normal(key, extent, jnp.float32)
    if split:
        array = array * steps_of(key, extent, split, -0.22, 0.18)
    return jnp.clip(array, -most, most).astype(held_as)


def setup_inputs(seed: int = 0) -> dict:
    seeds = jax.random.split(jax.random.key(seed), 13)
    return {
        "positions": scatter_about(seeds[0], (NROW, NCOL, 3, ATOMS), 1.0, 6.0, ((0, 4), (1, 16), (3, 4)), jnp.float32),
        "velocities": scatter_about(seeds[1], (NROW, NCOL, 3, ATOMS), 1.0, 6.0, ((0, 4), (1, 16), (3, 4)), jnp.float32),
        "inv_mass": jnp.clip(jnp.exp(math.log(2.0) - 1.3862944 * jax.random.uniform(seeds[2], (ATOMS,), jnp.float32) ** steps_of(seeds[2], (ATOMS,), ((0, 4),), -0.2, 0.2)), 0.5, 2.0),
        "cv_weight": scatter_about(seeds[3], (2, 3, ATOMS), ATOM_DEV ** -0.5, 0.125, ((2, 4),), jnp.float32),
        "stiffness": jnp.clip(jnp.exp(jax.random.uniform(seeds[4], (2,), jnp.float32, math.log(1.0), math.log(4.0))), 1.0, 4.0),
        "centers": jnp.clip(jax.random.uniform(seeds[5], (NROW, NCOL, 2), jnp.float32, -3.0, 3.0) * steps_of(seeds[5], (NROW, NCOL, 2), ((0, 4), (1, 16)), -0.4, 0.0), -3.0, 3.0),
        "block_order": draw_block_order(jax.random.fold_in(seeds[12], 71), 0),
        "pair_count": draw_pair_count(jax.random.fold_in(seeds[12], 71), 0),
        "pair_own": draw_pair_own(jax.random.fold_in(seeds[12], 71), 0),
        "pair_other": draw_pair_other(jax.random.fold_in(seeds[12], 71), 0),
        "accept_row": draw_accept_row(jax.random.fold_in(seeds[12], 71), 0),
        "accept_col": draw_accept_col(jax.random.fold_in(seeds[12], 71), 0),
    }


PAIR_EPS = 0.015625
DT = 0.1


def pair_tile(own_tile, other_tile):
    offsets = own_tile[:, :, None] - other_tile[:, None, :]
    squared = jnp.sum(offsets * offsets, axis=0)
    weight_tile = PAIR_EPS * jnp.exp(-0.5 * squared)
    return own_tile * jnp.sum(weight_tile, axis=1)[None, :] - jnp.dot(other_tile, weight_tile.T, precision=lax.Precision.HIGHEST)


def domain_forces(nearby, pair_total, own_blocks, other_blocks):
    blocks_dev = ATOM_DEV // BLK

    def add_tile(forces_acc, index):
        own_index = own_blocks[index]
        other_index = other_blocks[index]
        own_tile = lax.dynamic_slice(nearby, (jnp.int32(0), ((blocks_dev + own_index) * BLK).astype(jnp.int32)), (3, BLK))
        other_tile = lax.dynamic_slice(nearby, (jnp.int32(0), (other_index * BLK).astype(jnp.int32)), (3, BLK))
        live = (index < pair_total).astype(forces_acc.dtype)
        offset = (own_index * BLK).astype(jnp.int32)
        older = lax.dynamic_slice(forces_acc, (jnp.int32(0), offset), (3, BLK))
        forces_acc = lax.dynamic_update_slice(forces_acc, older + live * pair_tile(own_tile, other_tile), (jnp.int32(0), offset))
        return forces_acc, None

    forces_acc, _ = lax.scan(add_tile, jnp.zeros((3, ATOM_DEV), jnp.float32), jnp.arange(PMAX, dtype=jnp.int32))
    return forces_acc


def window_pair(coords, pair_count, pair_own, pair_other):
    domains = ATOMS // ATOM_DEV
    slab_rows = coords.reshape(3, domains, ATOM_DEV)
    zeros_slab = jnp.zeros((3, 1, ATOM_DEV), coords.dtype)
    padded = jnp.concatenate([zeros_slab, slab_rows, zeros_slab], axis=1)
    nearby = jnp.stack([padded[:, slab:slab + 3].reshape(3, 3 * ATOM_DEV) for slab in range(domains)])
    forces_all = jax.vmap(domain_forces)(nearby, pair_count, pair_own, pair_other)
    return jnp.transpose(forces_all, (1, 0, 2)).reshape(3, ATOMS)


def total_force(coords, weights, stiffness, centre_rows, pair_count, pair_own, pair_other):
    pair = jax.vmap(window_pair, in_axes=(0, None, None, None))(coords, pair_count, pair_own, pair_other)
    collective = jnp.sum(weights[None] * coords[:, None], axis=(2, 3))
    pull = stiffness[None, :] * (collective - centre_rows)
    return pair - jnp.sum(pull[:, :, None, None] * weights[None], axis=1)


def partner_select(state, flags, axis):
    count_axis = state.shape[axis]
    swapped = jnp.take(state, jnp.arange(count_axis, dtype=jnp.int32) ^ 1, axis=axis)
    return jnp.where((flags == 1)[:, :, None, None], swapped, state)


def reference(positions, velocities, inv_mass, cv_weight, stiffness, centers, block_order, pair_count, pair_own, pair_other, accept_row, accept_col):
    domains = ATOMS // ATOM_DEV
    windows = NROW * NCOL
    global_order = (block_order.reshape(domains, ATOM_DEV) + (jnp.arange(domains, dtype=jnp.int32) * ATOM_DEV)[:, None]).reshape(ATOMS).astype(jnp.int32)
    inverse = jnp.zeros((ATOMS,), jnp.int32).at[global_order].set(jnp.arange(ATOMS, dtype=jnp.int32))
    coords = positions.reshape(windows, 3, ATOMS)[:, :, global_order]
    speeds = velocities.reshape(windows, 3, ATOMS)[:, :, global_order]
    inverse_mass = inv_mass[global_order]
    weights = cv_weight[:, :, global_order]
    centre_rows = centers.reshape(windows, 2)
    forces_now = total_force(coords, weights, stiffness, centre_rows, pair_count, pair_own, pair_other)
    for _ in range(STEPS):
        speeds = speeds + (0.5 * DT) * inverse_mass * forces_now
        coords = coords + DT * speeds
        forces_now = total_force(coords, weights, stiffness, centre_rows, pair_count, pair_own, pair_other)
        speeds = speeds + (0.5 * DT) * inverse_mass * forces_now
    results = []
    for state in (coords, speeds, forces_now):
        state = state[:, :, inverse].reshape(NROW, NCOL, 3, ATOMS)
        state = partner_select(state, accept_row, 0)
        state = partner_select(state, accept_col, 1)
        results.append(state)
    return (results[0], results[1], results[2])
```

```python
import functools
import math

import jax
import jax.numpy as jnp
from jax import lax
from jax.experimental import pallas as pl
from jax.experimental.pallas import tpu as pltpu
from jax.sharding import PartitionSpec as P

BLK = 128
STEPS = 3
EVALS = STEPS + 1
LOG2_EPS = -6.0
DT = 0.1
KAPPA = math.sqrt(0.5 * math.log2(math.e))
MESH = pl.DeviceIdType.MESH
VMEM = pltpu.VMEM
SMEM = pltpu.SMEM


def lane_take(rows, lanes):
    dims = lax.GatherDimensionNumbers(
        offset_dims=(),
        collapsed_slice_dims=(1,),
        start_index_map=(1,),
        operand_batching_dims=(0,),
        start_indices_batching_dims=(0,),
    )
    return lax.gather(
        rows, lanes[..., None], dims, slice_sizes=(1, 1), mode=lax.GatherScatterMode.PROMISE_IN_BOUNDS
    )


def permuted(source_row, blocks, index):
    halves = []
    for half in range(blocks // 8):
        piece = index[half * 8:(half + 1) * 8]
        lanes = piece & (BLK - 1)
        owner = piece >> 7
        total = jnp.zeros((8, BLK), jnp.float32)
        for s in range(blocks):
            taken = lane_take(jnp.broadcast_to(source_row(s), (8, BLK)), lanes)
            total = jnp.where(owner == s, taken, total)
        halves.append(total)
    return jnp.concatenate(halves, axis=0)


def split3(value):
    high = value.astype(jnp.bfloat16)
    rest = value - high.astype(jnp.float32)
    mid = rest.astype(jnp.bfloat16)
    low = (rest - mid.astype(jnp.float32)).astype(jnp.bfloat16)
    return high, mid, low


def pair_rows(near, own, other):
    other_row = near[pl.ds(other, 1), :]
    stacked = jnp.concatenate(
        [other_row[:, c * BLK:(c + 1) * BLK] for c in range(3)] + [jnp.zeros((5, BLK), jnp.float32)], axis=0
    )
    columns = stacked.T
    own_row = near[pl.ds(own, 1), :]
    mine = [jnp.broadcast_to(own_row[:, c * BLK:(c + 1) * BLK], (8, BLK)) for c in range(3)]
    sums = [jnp.zeros((8, BLK), jnp.float32) for _ in range(3)]
    for k in range(BLK // 8):
        rows = columns[k * 8:(k + 1) * 8]
        offsets = [mine[c] - jnp.broadcast_to(rows[:, c:c + 1], (8, BLK)) for c in range(3)]
        power = LOG2_EPS - offsets[0] * offsets[0]
        power = power - offsets[1] * offsets[1]
        power = power - offsets[2] * offsets[2]
        weight = jnp.exp2(power)
        sums = [sums[c] + weight * offsets[c] for c in range(3)]
    return [jnp.sum(sums[c], axis=0, keepdims=True) for c in range(3)]


def simulate(
    domains,
    slots,
    positions,
    velocities,
    inv_mass,
    cv_weight,
    block_order,
    own_lanes,
    stiffness,
    centers,
    pair_count,
    accept_row,
    accept_col,
    pair_own,
    pair_other,
    state_out,
    inverse_out,
    raw_x,
    raw_v,
    meta,
    chosen,
    x_ref,
    v_ref,
    f_ref,
    near_0,
    near_1,
    near_2,
    near_3,
    weights,
    mass,
    table,
    tiles,
    partial,
    in_sem,
    swap_send,
    swap_recv,
    halo_send,
    halo_recv,
    cv_send,
    cv_recv,
):
    row = lax.axis_index("wrow")
    col = lax.axis_index("wcol")
    dom = lax.axis_index("dom")
    blocks = block_order.shape[0]
    nears = (near_0, near_1, near_2, near_3)
    partners = [
        {"wrow": row ^ 1},
        {"wcol": col ^ 1},
        {"wrow": row ^ 1, "wcol": col ^ 1},
    ]
    peers = [{"dom": lax.rem(dom + k, domains)} for k in range(1, domains)]

    barrier = pltpu.get_barrier_semaphore()
    for device in partners + peers:
        pl.semaphore_signal(barrier, inc=1, device_id=device, device_id_type=MESH)
    own_x = pltpu.make_async_copy(positions, raw_x.at[0], in_sem.at[0])
    own_v = pltpu.make_async_copy(velocities, raw_v.at[0], in_sem.at[1])
    own_x.start()
    own_v.start()

    line = lax.broadcasted_iota(jnp.int32, (8, BLK), 0)
    meta[0] = jnp.where(
        line == 0, centers[0:1, 0:1], jnp.where(line == 1, centers[0:1, 1:2], accept_row[...].astype(jnp.float32))
    )

    own_x.wait()
    pl.semaphore_wait(barrier, len(partners) + len(peers))

    def swap(buffer, which):
        return [
            pltpu.make_async_remote_copy(
                src_ref=buffer.at[0],
                dst_ref=buffer.at[k + 1],
                send_sem=swap_send.at[which, k],
                recv_sem=swap_recv.at[which, k],
                device_id=partners[k],
                device_id_type=MESH,
            )
            for k in (2, 0, 1)
        ]

    moved_x, moved_v, moved_meta = swap(raw_x, 0), swap(raw_v, 1), swap(meta, 2)
    for copy in moved_meta:
        copy.start()
    for copy in moved_x:
        copy.start()
    own_v.wait()
    for copy in moved_v:
        copy.start()

    order = block_order[...]
    for k in range(2):
        for c in range(3):
            weights[k, :, c * BLK:(c + 1) * BLK] = permuted(
                lambda s: cv_weight[(c * blocks + s) * 2 + k:(c * blocks + s) * 2 + k + 1, :], blocks, order
            )
    mass_now = permuted(lambda s: inv_mass[s:s + 1, :], blocks, order)
    for c in range(3):
        mass[:, c * BLK:(c + 1) * BLK] = mass_now

    lane = lax.broadcasted_iota(jnp.int32, (blocks, BLK), 1)
    hi_line = lax.broadcasted_iota(jnp.int32, (blocks, BLK), 0)
    lo_line = lax.broadcasted_iota(jnp.int32, (BLK, BLK), 0)
    found = jnp.zeros((2 * blocks, BLK), jnp.float32)
    for b in range(blocks):
        atoms = order[b:b + 1]
        here = hi_line == (atoms >> 7)
        left = jnp.concatenate(
            [
                jnp.where(here, b, 0).astype(jnp.float32).astype(jnp.bfloat16),
                jnp.where(here, lane, 0).astype(jnp.float32).astype(jnp.bfloat16),
            ],
            axis=0,
        )
        right = jnp.where(lo_line == (atoms & (BLK - 1)), 1.0, 0.0).astype(jnp.bfloat16)
        found = found + lax.dot_general(left, right, (((1,), (1,)), ((), ())), preferred_element_type=jnp.float32)
    inverse_out[...] = (found[:blocks] * BLK + found[blocks:]).astype(jnp.int32)

    slot_lane = lax.broadcasted_iota(jnp.int32, (blocks, slots), 1)
    slot_line = lax.broadcasted_iota(jnp.int32, (blocks, slots), 0)
    listed = (own_lanes[...] == slot_line) & (slot_lane < pair_count[...])
    table[...] = jnp.where(listed, 1.0, 0.0).astype(jnp.bfloat16)

    for copy in moved_meta:
        copy.wait_recv()

    def choose(read):
        here = read(0)
        own_flag, col_flag = (jnp.broadcast_to(meta[k, 2:3, :], here.shape) for k in (0, 2))
        taken = jnp.broadcast_to(accept_col[...], here.shape)
        mine = jnp.where(own_flag == 1.0, read(1), here)
        theirs = jnp.where(col_flag == 1.0, read(3), read(2))
        return jnp.where(taken == 1, theirs, mine)

    def choose_all(buffer, target):
        chosen[...] = choose(lambda k: buffer[k])
        for c in range(3):
            target[:, c * BLK:(c + 1) * BLK] = permuted(
                lambda s: chosen[c * blocks + s:c * blocks + s + 1, :], blocks, order
            )

    centre = choose(lambda k: meta[k])

    for copy in moved_x:
        copy.wait_recv()
    choose_all(raw_x, x_ref)

    def halo(t):
        mine = nears[t].at[pl.ds(blocks, blocks), :]
        down = pltpu.make_async_remote_copy(
            src_ref=mine,
            dst_ref=nears[t].at[pl.ds(2 * blocks, blocks), :],
            send_sem=halo_send.at[t, 0],
            recv_sem=halo_recv.at[t, 0],
            device_id={"dom": lax.max(dom - 1, 0)},
            device_id_type=MESH,
        )
        up = pltpu.make_async_remote_copy(
            src_ref=mine,
            dst_ref=nears[t].at[pl.ds(0, blocks), :],
            send_sem=halo_send.at[t, 1],
            recv_sem=halo_recv.at[t, 1],
            device_id={"dom": lax.min(dom + 1, domains - 1)},
            device_id_type=MESH,
        )
        return down, up

    def shares(t):
        return [
            pltpu.make_async_remote_copy(
                src_ref=partial.at[t, 0],
                dst_ref=partial.at[t, k + 1],
                send_sem=cv_send.at[t, k],
                recv_sem=cv_recv.at[t, k],
                device_id=peers[k],
                device_id_type=MESH,
            )
            for k in range(domains - 1)
        ]

    has_lower = dom > 0
    has_upper = dom < domains - 1

    for t in range(EVALS):
        if t > 0:
            speeds = v_ref[...] + (0.5 * DT) * mass[...] * f_ref[...]
            v_ref[...] = speeds
            x_ref[...] = x_ref[...] + DT * speeds
        now = x_ref[...]
        nears[t][blocks:2 * blocks, :] = KAPPA * now
        down, up = halo(t)
        pl.when(has_lower)(down.start)
        pl.when(has_upper)(up.start)
        for k in range(2):
            product = weights[k] * now
            folded = product[:8] + product[8:]
            partial[t, 0, k * 8:(k + 1) * 8, :] = (
                folded[:, :BLK] + folded[:, BLK:2 * BLK] + folded[:, 2 * BLK:]
            )
        sent = shares(t)
        for copy in sent:
            copy.start()
        if t == 0:
            for copy in moved_v:
                copy.wait_recv()
            choose_all(raw_v, v_ref)
        pl.when(has_lower)(up.wait_recv)
        pl.when(has_upper)(down.wait_recv)

        def add_tile(p, carry):
            rows = pair_rows(nears[t], pair_own[0, p] + blocks, pair_other[0, p])
            for c in range(3):
                tiles[c, pl.ds(p, 1), :] = rows[c]
            return carry

        lax.fori_loop(0, slots, add_tile, 0, unroll=2)
        pair = jnp.zeros((blocks, 3 * BLK), jnp.float32)
        for piece in split3(jnp.concatenate([tiles[c] for c in range(3)], axis=1)):
            pair = pair + jnp.dot(table[...], piece, preferred_element_type=jnp.float32)
        force = (1.0 / KAPPA) * pair
        for copy in sent:
            copy.wait_recv()
        share = partial[t, 0]
        for k in range(1, domains):
            share = share + partial[t, k]
        for k in range(2):
            value = jnp.sum(
                jnp.sum(share[k * 8:(k + 1) * 8], axis=0, keepdims=True), axis=1, keepdims=True
            )
            force = force - (stiffness[0:1, k:k + 1] * (value - centre[k:k + 1, 0:1])) * weights[k]
        f_ref[...] = force
        if t > 0:
            v_ref[...] = v_ref[...] + (0.5 * DT) * mass[...] * force

    state_out[0:blocks, :] = x_ref[...]
    state_out[blocks:2 * blocks, :] = v_ref[...]
    state_out[2 * blocks:3 * blocks, :] = f_ref[...]

    for copy in moved_meta + moved_x + moved_v:
        copy.wait_send()
    for t in range(EVALS):
        down, up = halo(t)
        pl.when(has_lower)(down.wait_send)
        pl.when(has_upper)(up.wait_send)
        for copy in shares(t):
            copy.wait_send()


def restore(state, inverse, x_out, v_out, f_out):
    blocks = inverse.shape[0]
    index = inverse[...]
    for a, out in enumerate((x_out, v_out, f_out)):
        for c in range(3):
            value = permuted(
                lambda s: state[a * blocks + s:a * blocks + s + 1, c * BLK:(c + 1) * BLK], blocks, index
            )
            out[c * blocks:(c + 1) * blocks, :] = value


def per_device(
    domains,
    positions,
    velocities,
    inv_mass,
    cv_weight,
    stiffness,
    centers,
    block_order,
    pair_count,
    pair_own,
    pair_other,
    accept_row,
    accept_col,
):
    atoms = block_order.shape[0]
    blocks = atoms // BLK
    slots = pair_own.shape[1]
    f32 = jnp.float32
    vmem = pl.BlockSpec(memory_space=VMEM)
    smem = pl.BlockSpec(memory_space=SMEM)
    anywhere = pl.BlockSpec(memory_space=pl.ANY)
    dma = pltpu.SemaphoreType.DMA
    wide = 3 * BLK
    state, inverse = pl.pallas_call(
        functools.partial(simulate, domains, slots),
        out_shape=(
            jax.ShapeDtypeStruct((3 * blocks, wide), f32),
            jax.ShapeDtypeStruct((blocks, BLK), jnp.int32),
        ),
        in_specs=[anywhere] * 2 + [vmem] * 9 + [smem] * 2,
        out_specs=(vmem, vmem),
        scratch_shapes=[
            VMEM((4, 3 * blocks, BLK), f32),
            VMEM((4, 3 * blocks, BLK), f32),
            VMEM((4, 8, BLK), f32),
            VMEM((3 * blocks, BLK), f32),
            VMEM((blocks, wide), f32),
            VMEM((blocks, wide), f32),
            VMEM((blocks, wide), f32),
            VMEM((3 * blocks, wide), f32),
            VMEM((3 * blocks, wide), f32),
            VMEM((3 * blocks, wide), f32),
            VMEM((3 * blocks, wide), f32),
            VMEM((2, blocks, wide), f32),
            VMEM((blocks, wide), f32),
            VMEM((blocks, slots), jnp.bfloat16),
            VMEM((3, slots, BLK), f32),
            VMEM((EVALS, domains, 16, BLK), f32),
            dma((2,)),
            dma((3, 3)),
            dma((3, 3)),
            dma((EVALS, 2)),
            dma((EVALS, 2)),
            dma((EVALS, domains - 1)),
            dma((EVALS, domains - 1)),
        ],
        compiler_params=pltpu.CompilerParams(collective_id=0, has_side_effects=True),
        name="simulate",
    )(
        positions.reshape(3 * blocks, BLK),
        velocities.reshape(3 * blocks, BLK),
        inv_mass.reshape(blocks, BLK),
        cv_weight.reshape(2, 3, blocks, BLK).transpose(1, 2, 0, 3).reshape(6 * blocks, BLK),
        block_order.reshape(blocks, BLK),
        pair_own,
        stiffness[None],
        centers[0],
        pair_count[None],
        accept_row,
        accept_col,
        pair_own,
        pair_other,
    )
    outs = pl.pallas_call(
        restore,
        out_shape=(jax.ShapeDtypeStruct((3 * blocks, BLK), f32),) * 3,
        in_specs=[vmem] * 2,
        out_specs=(vmem,) * 3,
        name="restore",
    )(state, inverse)
    return tuple(out.reshape(1, 1, 3, atoms) for out in outs)


def solution(mesh):
    placed = (
        P("wrow", "wcol", None, "dom"),
        P("wrow", "wcol", None, "dom"),
        P("dom"),
        P(None, None, "dom"),
        P(),
        P("wrow", "wcol", None),
        P("dom"),
        P("dom"),
        P("dom", None),
        P("dom", None),
        P("wrow", "wcol"),
        P("wrow", "wcol"),
    )
    return jax.shard_map(
        functools.partial(per_device, mesh.shape["dom"]),
        mesh=mesh,
        in_specs=placed,
        out_specs=(P("wrow", "wcol", None, "dom"),) * 3,
        check_vma=False,
    )
```

```python
import functools
import math

import jax
import jax.numpy as jnp
from jax import lax
from jax.experimental import pallas as pl
from jax.experimental.pallas import tpu as pltpu
from jax.sharding import PartitionSpec as P

BLK = 128
STEPS = 3
EVALS = STEPS + 1
UNROLL = 16
LOG2_EPS = -6.0
DT = 0.1
KAPPA = math.sqrt(math.log2(math.e))
MESH = pl.DeviceIdType.MESH
VMEM = pltpu.VMEM
SMEM = pltpu.SMEM


def lane_take(rows, lanes):
    dims = lax.GatherDimensionNumbers(
        offset_dims=(),
        collapsed_slice_dims=(1,),
        start_index_map=(1,),
        operand_batching_dims=(0,),
        start_indices_batching_dims=(0,),
    )
    return lax.gather(
        rows, lanes[..., None], dims, slice_sizes=(1, 1), mode=lax.GatherScatterMode.PROMISE_IN_BOUNDS
    )


def permuted(source_row, blocks, index):
    halves = []
    for half in range(blocks // 8):
        piece = index[half * 8:(half + 1) * 8]
        lanes = piece & (BLK - 1)
        owner = piece >> 7
        total = jnp.zeros((8, BLK), jnp.float32)
        for s in range(blocks):
            taken = lane_take(jnp.broadcast_to(source_row(s), (8, BLK)), lanes)
            total = jnp.where(owner == s, taken, total)
        halves.append(total)
    return jnp.concatenate(halves, axis=0)


def split3(value):
    high = value.astype(jnp.bfloat16)
    rest = value - high.astype(jnp.float32)
    mid = rest.astype(jnp.bfloat16)
    low = (rest - mid.astype(jnp.float32)).astype(jnp.bfloat16)
    return high, mid, low


def split2(value):
    high = value.astype(jnp.bfloat16)
    return high, (value - high.astype(jnp.float32)).astype(jnp.bfloat16)


def stack_groups(groups):
    zero = jnp.zeros((8, BLK), jnp.float32)
    upper = jnp.concatenate(groups[:2], axis=0).astype(jnp.bfloat16)
    lower = jnp.concatenate([groups[2], zero], axis=0).astype(jnp.bfloat16)
    return jnp.concatenate([upper, lower], axis=0)


def parts(value):
    return [piece.astype(jnp.float32) for piece in split3(value)]


def partner_rows(rows, line):
    high, mid, low = parts(rows)
    middle = (line > 3) & (line < 7)
    return stack_groups(
        [
            high,
            jnp.where(line < 4, mid, jnp.where(line == 7, high, low)),
            jnp.where(line == 3, low, jnp.where(middle, mid, high)),
        ]
    )


def owner_rows(rows, line):
    high, mid, low = parts(rows)
    middle = (line > 3) & (line < 7)
    return stack_groups(
        [
            jnp.where(middle, mid, high),
            jnp.where(line == 7, mid, high),
            jnp.where(line == 3, high, jnp.where(middle, mid, low)),
        ]
    )


def two_tiles(partners, owners, other, own):
    left = [partners[q] for q in other]
    right = [owners[b] for b in own]
    zero = jnp.zeros_like(right[0])
    power = lax.dot_general(
        jnp.concatenate(left, axis=0),
        jnp.concatenate(
            [jnp.concatenate([right[0], zero], axis=1), jnp.concatenate([zero, right[1]], axis=1)], axis=0
        ),
        (((0,), (0,)), ((), ())),
        preferred_element_type=jnp.float32,
    )
    weight = jnp.concatenate(split2(jnp.exp2(jnp.minimum(power, LOG2_EPS))), axis=0)
    heads = [jnp.concatenate([rows[:16], rows[:16]], axis=1) for rows in left]
    sums = jnp.dot(jnp.concatenate(heads, axis=0), weight, preferred_element_type=jnp.float32)
    return sums[:16, :BLK], sums[16:, BLK:]


def simulate(
    domains,
    slots,
    positions,
    velocities,
    inv_mass,
    cv_weight,
    block_order,
    own_lanes,
    stiffness,
    centers,
    pair_count,
    accept_row,
    accept_col,
    pair_own,
    pair_other,
    state_out,
    inverse_out,
    raw_x,
    raw_v,
    meta,
    chosen,
    x_ref,
    v_ref,
    f_ref,
    near_0,
    near_1,
    near_2,
    near_3,
    weights,
    mass,
    table,
    tiles,
    partners_tab,
    owners_tab,
    partial,
    in_sem,
    swap_send,
    swap_recv,
    halo_send,
    halo_recv,
    cv_send,
    cv_recv,
):
    row = lax.axis_index("wrow")
    col = lax.axis_index("wcol")
    dom = lax.axis_index("dom")
    blocks = block_order.shape[0]
    rows_slab = 4 * blocks
    nears = (near_0, near_1, near_2, near_3)
    partners = [
        {"wrow": row ^ 1},
        {"wcol": col ^ 1},
        {"wrow": row ^ 1, "wcol": col ^ 1},
    ]
    peers = [{"dom": lax.rem(dom + k, domains)} for k in range(1, domains)]

    barrier = pltpu.get_barrier_semaphore()
    for device in partners + peers:
        pl.semaphore_signal(barrier, inc=1, device_id=device, device_id_type=MESH)
    own_x = pltpu.make_async_copy(positions, raw_x.at[0], in_sem.at[0])
    own_v = pltpu.make_async_copy(velocities, raw_v.at[0], in_sem.at[1])
    own_x.start()
    own_v.start()

    line = lax.broadcasted_iota(jnp.int32, (8, BLK), 0)
    meta[0] = jnp.where(
        line == 0, centers[0:1, 0:1], jnp.where(line == 1, centers[0:1, 1:2], accept_row[...].astype(jnp.float32))
    )

    own_x.wait()
    pl.semaphore_wait(barrier, len(partners) + len(peers))

    def swap(buffer, which):
        return [
            pltpu.make_async_remote_copy(
                src_ref=buffer.at[0],
                dst_ref=buffer.at[k + 1],
                send_sem=swap_send.at[which, k],
                recv_sem=swap_recv.at[which, k],
                device_id=partners[k],
                device_id_type=MESH,
            )
            for k in (2, 0, 1)
        ]

    moved_x, moved_v, moved_meta = swap(raw_x, 0), swap(raw_v, 1), swap(meta, 2)
    for copy in moved_meta:
        copy.start()
    for copy in moved_x:
        copy.start()
    own_v.wait()
    for copy in moved_v:
        copy.start()

    order = block_order[...]
    for k in range(2):
        for c in range(3):
            weights[k, :, c * BLK:(c + 1) * BLK] = permuted(
                lambda s: cv_weight[(c * blocks + s) * 2 + k:(c * blocks + s) * 2 + k + 1, :], blocks, order
            )
    mass_now = permuted(lambda s: inv_mass[s:s + 1, :], blocks, order)
    for c in range(3):
        mass[:, c * BLK:(c + 1) * BLK] = mass_now

    lane = lax.broadcasted_iota(jnp.int32, (blocks, BLK), 1)
    hi_line = lax.broadcasted_iota(jnp.int32, (blocks, BLK), 0)
    lo_line = lax.broadcasted_iota(jnp.int32, (BLK, BLK), 0)
    found = jnp.zeros((2 * blocks, BLK), jnp.float32)
    for b in range(blocks):
        atoms = order[b:b + 1]
        here = hi_line == (atoms >> 7)
        left = jnp.concatenate(
            [
                jnp.where(here, b, 0).astype(jnp.float32).astype(jnp.bfloat16),
                jnp.where(here, lane, 0).astype(jnp.float32).astype(jnp.bfloat16),
            ],
            axis=0,
        )
        right = jnp.where(lo_line == (atoms & (BLK - 1)), 1.0, 0.0).astype(jnp.bfloat16)
        found = found + lax.dot_general(left, right, (((1,), (1,)), ((), ())), preferred_element_type=jnp.float32)
    inverse_out[...] = (found[:blocks] * BLK + found[blocks:]).astype(jnp.int32)

    slot_lane = lax.broadcasted_iota(jnp.int32, (blocks, slots), 1)
    slot_line = lax.broadcasted_iota(jnp.int32, (blocks, slots), 0)
    listed = (own_lanes[...] == slot_line) & (slot_lane < pair_count[...])
    table[...] = jnp.where(listed, 1.0, 0.0).astype(jnp.bfloat16)

    for copy in moved_meta:
        copy.wait_recv()

    def choose(read):
        here = read(0)
        own_flag, col_flag = (jnp.broadcast_to(meta[k, 2:3, :], here.shape) for k in (0, 2))
        taken = jnp.broadcast_to(accept_col[...], here.shape)
        mine = jnp.where(own_flag == 1.0, read(1), here)
        theirs = jnp.where(col_flag == 1.0, read(3), read(2))
        return jnp.where(taken == 1, theirs, mine)

    def choose_all(buffer, target):
        chosen[...] = choose(lambda k: buffer[k])
        for c in range(3):
            target[:, c * BLK:(c + 1) * BLK] = permuted(
                lambda s: chosen[c * blocks + s:c * blocks + s + 1, :], blocks, order
            )

    centre = choose(lambda k: meta[k])

    for copy in moved_x:
        copy.wait_recv()
    choose_all(raw_x, x_ref)

    def halo(t):
        mine = nears[t].at[pl.ds(rows_slab, rows_slab), :]
        down = pltpu.make_async_remote_copy(
            src_ref=mine,
            dst_ref=nears[t].at[pl.ds(2 * rows_slab, rows_slab), :],
            send_sem=halo_send.at[t, 0],
            recv_sem=halo_recv.at[t, 0],
            device_id={"dom": lax.max(dom - 1, 0)},
            device_id_type=MESH,
        )
        up = pltpu.make_async_remote_copy(
            src_ref=mine,
            dst_ref=nears[t].at[pl.ds(0, rows_slab), :],
            send_sem=halo_send.at[t, 1],
            recv_sem=halo_recv.at[t, 1],
            device_id={"dom": lax.min(dom + 1, domains - 1)},
            device_id_type=MESH,
        )
        return down, up

    def shares(t):
        return [
            pltpu.make_async_remote_copy(
                src_ref=partial.at[t, 0],
                dst_ref=partial.at[t, k + 1],
                send_sem=cv_send.at[t, k],
                recv_sem=cv_recv.at[t, k],
                device_id=peers[k],
                device_id_type=MESH,
            )
            for k in range(domains - 1)
        ]

    has_lower = dom > 0
    has_upper = dom < domains - 1

    for t in range(EVALS):
        if t > 0:
            speeds = v_ref[...] + (0.5 * DT) * mass[...] * f_ref[...]
            v_ref[...] = speeds
            x_ref[...] = x_ref[...] + DT * speeds
        now = x_ref[...]
        scaled = [KAPPA * now[:, c * BLK:(c + 1) * BLK] for c in range(3)]
        norm = -0.5 * (scaled[0] * scaled[0] + scaled[1] * scaled[1] + scaled[2] * scaled[2])
        for c, rows in enumerate(scaled + [norm]):
            nears[t][pl.ds(rows_slab + c, blocks, stride=4), :] = rows
        down, up = halo(t)
        pl.when(has_lower)(down.start)
        pl.when(has_upper)(up.start)
        for k in range(2):
            product = weights[k] * now
            folded = product[:8] + product[8:]
            partial[t, 0, k * 8:(k + 1) * 8, :] = (
                folded[:, :BLK] + folded[:, BLK:2 * BLK] + folded[:, 2 * BLK:]
            )
        sent = shares(t)
        for copy in sent:
            copy.start()
        if t == 0:
            for copy in moved_v:
                copy.wait_recv()
            choose_all(raw_v, v_ref)

        def block_rows(b):
            four = nears[t][4 * b:4 * b + 4, :]
            return jnp.concatenate([four, four], axis=0)

        for b in range(blocks):
            rows = block_rows(blocks + b)
            partners_tab[blocks + b] = partner_rows(jnp.where(line == 7, 1.0, rows), line)
            owners_tab[b] = owner_rows(
                jnp.where(line == 3, 1.0, jnp.where(line == 7, rows + LOG2_EPS, rows)), line
            )
        pl.when(has_lower)(up.wait_recv)
        pl.when(has_upper)(down.wait_recv)
        for b in list(range(blocks)) + list(range(2 * blocks, 3 * blocks)):
            partners_tab[b] = partner_rows(jnp.where(line == 7, 1.0, block_rows(b)), line)

        def add_tiles(group, carry):
            for u in range(UNROLL):
                first = group * (2 * UNROLL) + 2 * u
                sums = two_tiles(
                    partners_tab,
                    owners_tab,
                    [pair_other[0, first + k] for k in range(2)],
                    [pair_own[0, first + k] for k in range(2)],
                )
                for k in range(2):
                    tiles[pl.ds(pl.multiple_of(16 * (first + k), 16), 16), :] = sums[k]
            return carry

        lax.fori_loop(0, slots // (2 * UNROLL), add_tiles, 0)

        def slot_rows(r):
            return tiles[pl.ds(r, slots, stride=16), :]

        listed_rows = jnp.concatenate(
            [slot_rows(c) + slot_rows(8 + c) + slot_rows(12 + c) for c in range(3)] + [slot_rows(7)], axis=1
        )
        pair = jnp.zeros((blocks, 4 * BLK), jnp.float32)
        for piece in split3(listed_rows):
            pair = pair + jnp.dot(table[...], piece, preferred_element_type=jnp.float32)
        total = pair[:, 3 * BLK:]
        force = now * jnp.concatenate([total, total, total], axis=1) - (1.0 / KAPPA) * pair[:, :3 * BLK]
        for copy in sent:
            copy.wait_recv()
        share = partial[t, 0]
        for k in range(1, domains):
            share = share + partial[t, k]
        for k in range(2):
            value = jnp.sum(
                jnp.sum(share[k * 8:(k + 1) * 8], axis=0, keepdims=True), axis=1, keepdims=True
            )
            force = force - (stiffness[0:1, k:k + 1] * (value - centre[k:k + 1, 0:1])) * weights[k]
        f_ref[...] = force
        if t > 0:
            v_ref[...] = v_ref[...] + (0.5 * DT) * mass[...] * force

    state_out[0:blocks, :] = x_ref[...]
    state_out[blocks:2 * blocks, :] = v_ref[...]
    state_out[2 * blocks:3 * blocks, :] = f_ref[...]

    for copy in moved_meta + moved_x + moved_v:
        copy.wait_send()
    for t in range(EVALS):
        down, up = halo(t)
        pl.when(has_lower)(down.wait_send)
        pl.when(has_upper)(up.wait_send)
        for copy in shares(t):
            copy.wait_send()


def restore(state, inverse, x_out, v_out, f_out):
    blocks = inverse.shape[0]
    index = inverse[...]
    for a, out in enumerate((x_out, v_out, f_out)):
        for c in range(3):
            value = permuted(
                lambda s: state[a * blocks + s:a * blocks + s + 1, c * BLK:(c + 1) * BLK], blocks, index
            )
            out[c * blocks:(c + 1) * blocks, :] = value


def per_device(
    domains,
    positions,
    velocities,
    inv_mass,
    cv_weight,
    stiffness,
    centers,
    block_order,
    pair_count,
    pair_own,
    pair_other,
    accept_row,
    accept_col,
):
    atoms = block_order.shape[0]
    blocks = atoms // BLK
    slots = pair_own.shape[1]
    f32 = jnp.float32
    vmem = pl.BlockSpec(memory_space=VMEM)
    smem = pl.BlockSpec(memory_space=SMEM)
    anywhere = pl.BlockSpec(memory_space=pl.ANY)
    dma = pltpu.SemaphoreType.DMA
    wide = 3 * BLK
    state, inverse = pl.pallas_call(
        functools.partial(simulate, domains, slots),
        out_shape=(
            jax.ShapeDtypeStruct((3 * blocks, wide), f32),
            jax.ShapeDtypeStruct((blocks, BLK), jnp.int32),
        ),
        in_specs=[anywhere] * 2 + [vmem] * 9 + [smem] * 2,
        out_specs=(vmem, vmem),
        scratch_shapes=[
            VMEM((4, 3 * blocks, BLK), f32),
            VMEM((4, 3 * blocks, BLK), f32),
            VMEM((4, 8, BLK), f32),
            VMEM((3 * blocks, BLK), f32),
            VMEM((blocks, wide), f32),
            VMEM((blocks, wide), f32),
            VMEM((blocks, wide), f32),
            VMEM((12 * blocks, BLK), f32),
            VMEM((12 * blocks, BLK), f32),
            VMEM((12 * blocks, BLK), f32),
            VMEM((12 * blocks, BLK), f32),
            VMEM((2, blocks, wide), f32),
            VMEM((blocks, wide), f32),
            VMEM((blocks, slots), jnp.bfloat16),
            VMEM((16 * slots, BLK), f32),
            VMEM((3 * blocks, 32, BLK), jnp.bfloat16),
            VMEM((blocks, 32, BLK), jnp.bfloat16),
            VMEM((EVALS, domains, 16, BLK), f32),
            dma((2,)),
            dma((3, 3)),
            dma((3, 3)),
            dma((EVALS, 2)),
            dma((EVALS, 2)),
            dma((EVALS, domains - 1)),
            dma((EVALS, domains - 1)),
        ],
        compiler_params=pltpu.CompilerParams(collective_id=0, has_side_effects=True),
        name="simulate",
    )(
        positions.reshape(3 * blocks, BLK),
        velocities.reshape(3 * blocks, BLK),
        inv_mass.reshape(blocks, BLK),
        cv_weight.reshape(2, 3, blocks, BLK).transpose(1, 2, 0, 3).reshape(6 * blocks, BLK),
        block_order.reshape(blocks, BLK),
        pair_own,
        stiffness[None],
        centers[0],
        pair_count[None],
        accept_row,
        accept_col,
        pair_own,
        pair_other,
    )
    outs = pl.pallas_call(
        restore,
        out_shape=(jax.ShapeDtypeStruct((3 * blocks, BLK), f32),) * 3,
        in_specs=[vmem] * 2,
        out_specs=(vmem,) * 3,
        name="restore",
    )(state, inverse)
    return tuple(out.reshape(1, 1, 3, atoms) for out in outs)


def solution(mesh):
    placed = (
        P("wrow", "wcol", None, "dom"),
        P("wrow", "wcol", None, "dom"),
        P("dom"),
        P(None, None, "dom"),
        P(),
        P("wrow", "wcol", None),
        P("dom"),
        P("dom"),
        P("dom", None),
        P("dom", None),
        P("wrow", "wcol"),
        P("wrow", "wcol"),
    )
    return jax.shard_map(
        functools.partial(per_device, mesh.shape["dom"]),
        mesh=mesh,
        in_specs=placed,
        out_specs=(P("wrow", "wcol", None, "dom"),) * 3,
        check_vma=False,
    )
```

```python
import functools
import math

import jax
import jax.numpy as jnp
from jax import lax
from jax.experimental import pallas as pl
from jax.experimental.pallas import tpu as pltpu
from jax.sharding import PartitionSpec as P

BLK = 128
STEPS = 3
EVALS = STEPS + 1
UNROLL = 32
LOG2_EPS = -6.0
DT = 0.1
KAPPA = math.sqrt(math.log2(math.e))
MESH = pl.DeviceIdType.MESH
VMEM = pltpu.VMEM
SMEM = pltpu.SMEM


def lane_take(rows, lanes):
    dims = lax.GatherDimensionNumbers(
        offset_dims=(),
        collapsed_slice_dims=(1,),
        start_index_map=(1,),
        operand_batching_dims=(0,),
        start_indices_batching_dims=(0,),
    )
    return lax.gather(
        rows, lanes[..., None], dims, slice_sizes=(1, 1), mode=lax.GatherScatterMode.PROMISE_IN_BOUNDS
    )


def permuted(source_row, blocks, index):
    halves = []
    for half in range(blocks // 8):
        piece = index[half * 8:(half + 1) * 8]
        lanes = piece & (BLK - 1)
        owner = piece >> 7
        total = jnp.zeros((8, BLK), jnp.float32)
        for s in range(blocks):
            taken = lane_take(jnp.broadcast_to(source_row(s), (8, BLK)), lanes)
            total = jnp.where(owner == s, taken, total)
        halves.append(total)
    return jnp.concatenate(halves, axis=0)


def split3(value):
    high = value.astype(jnp.bfloat16)
    rest = value - high.astype(jnp.float32)
    mid = rest.astype(jnp.bfloat16)
    low = (rest - mid.astype(jnp.float32)).astype(jnp.bfloat16)
    return high, mid, low


def split2(value):
    high = value.astype(jnp.bfloat16)
    return high, (value - high.astype(jnp.float32)).astype(jnp.bfloat16)


def stack_groups(groups):
    zero = jnp.zeros((8, BLK), jnp.float32)
    upper = jnp.concatenate(groups[:2], axis=0).astype(jnp.bfloat16)
    lower = jnp.concatenate([groups[2], zero], axis=0).astype(jnp.bfloat16)
    return jnp.concatenate([upper, lower], axis=0)


def parts(value):
    return [piece.astype(jnp.float32) for piece in split3(value)]


def partner_rows(rows, line):
    high, mid, low = parts(rows)
    middle = (line > 3) & (line < 7)
    return stack_groups(
        [
            high,
            jnp.where(line < 4, mid, jnp.where(line == 7, high, low)),
            jnp.where(line == 3, low, jnp.where(middle, mid, high)),
        ]
    )


def owner_rows(rows, line):
    high, mid, low = parts(rows)
    middle = (line > 3) & (line < 7)
    return stack_groups(
        [
            jnp.where(middle, mid, high),
            jnp.where(line == 7, mid, high),
            jnp.where(line == 3, high, jnp.where(middle, mid, low)),
        ]
    )


def two_tiles(partners, owners, other, own):
    left = [partners[q] for q in other]
    right = [owners[b] for b in own]
    zero = jnp.zeros_like(right[0])
    power = lax.dot_general(
        jnp.concatenate(left, axis=0),
        jnp.concatenate(
            [jnp.concatenate([right[0], zero], axis=1), jnp.concatenate([zero, right[1]], axis=1)], axis=0
        ),
        (((0,), (0,)), ((), ())),
        preferred_element_type=jnp.float32,
    )
    weight = jnp.concatenate(split2(jnp.exp2(jnp.minimum(power, LOG2_EPS))), axis=0)
    heads = [jnp.concatenate([rows[:16], rows[:16]], axis=1) for rows in left]
    sums = jnp.dot(jnp.concatenate(heads, axis=0), weight, preferred_element_type=jnp.float32)
    return sums[:16, :BLK], sums[16:, BLK:]


def simulate(domains, slots, *refs):
    inputs, refs = refs[:13], refs[13:]
    (state_out, inverse_out), refs = refs[:2], refs[2:]
    local, refs = refs[:11], refs[11:]
    inv_mass, cv_weight, block_order, own_lanes, stiffness, centers, pair_count = local[:7]
    accept_row, accept_col, pair_own, pair_other = local[7:]
    raw_x, raw_v, meta, chosen, x_ref, v_ref, f_ref, near = refs[:8]
    weights, mass, table, tiles, partners_tab, owners_tab, partial = refs[8:15]
    in_sem, swap_send, swap_recv, halo_send, halo_recv, cv_send, cv_recv = refs[15:]
    row = lax.axis_index("wrow")
    col = lax.axis_index("wcol")
    dom = lax.axis_index("dom")
    blocks = block_order.shape[0]
    rows_slab = 4 * blocks
    partners = [
        {"wrow": row ^ 1},
        {"wcol": col ^ 1},
        {"wrow": row ^ 1, "wcol": col ^ 1},
    ]
    peers = [{"dom": lax.rem(dom + k, domains)} for k in range(1, domains)]

    barrier = pltpu.get_barrier_semaphore()
    for device in partners + peers:
        pl.semaphore_signal(barrier, inc=1, device_id=device, device_id_type=MESH)
    arrivals = [
        pltpu.make_async_copy(source, target, in_sem.at[k])
        for k, (source, target) in enumerate(zip(inputs, (raw_x.at[0], raw_v.at[0]) + local))
    ]
    for k in (0, 7, 9, 1, 4, 2, 3, 5, 6, 8, 10, 11, 12):
        arrivals[k].start()
    own_x, own_v = arrivals[:2]
    arrivals[7].wait()
    arrivals[9].wait()

    line = lax.broadcasted_iota(jnp.int32, (8, BLK), 0)
    meta[0] = jnp.where(
        line == 0, centers[0:1, 0:1], jnp.where(line == 1, centers[0:1, 1:2], accept_row[...].astype(jnp.float32))
    )

    own_x.wait()
    pl.semaphore_wait(barrier, len(partners) + len(peers))

    def swap(buffer, which):
        return [
            pltpu.make_async_remote_copy(
                src_ref=buffer.at[0],
                dst_ref=buffer.at[k + 1],
                send_sem=swap_send.at[which, k],
                recv_sem=swap_recv.at[which, k],
                device_id=partners[k],
                device_id_type=MESH,
            )
            for k in (2, 0, 1)
        ]

    moved_x, moved_v, moved_meta = swap(raw_x, 0), swap(raw_v, 1), swap(meta, 2)
    for copy in moved_meta:
        copy.start()
    for copy in moved_x:
        copy.start()
    own_v.wait()
    for copy in moved_v:
        copy.start()

    for k in (4, 2, 3, 5, 6, 8, 10, 11, 12):
        arrivals[k].wait()
    order = block_order[...]
    for k in range(2):
        for c in range(3):
            weights[k, :, c * BLK:(c + 1) * BLK] = permuted(
                lambda s: cv_weight[(c * blocks + s) * 2 + k:(c * blocks + s) * 2 + k + 1, :], blocks, order
            )
    mass_now = permuted(lambda s: inv_mass[s:s + 1, :], blocks, order)
    for c in range(3):
        mass[:, c * BLK:(c + 1) * BLK] = mass_now

    lane = lax.broadcasted_iota(jnp.int32, (blocks, BLK), 1)
    hi_line = lax.broadcasted_iota(jnp.int32, (blocks, BLK), 0)
    lo_line = lax.broadcasted_iota(jnp.int32, (BLK, BLK), 0)
    found = jnp.zeros((2 * blocks, BLK), jnp.float32)
    for b in range(blocks):
        atoms = order[b:b + 1]
        here = hi_line == (atoms >> 7)
        left = jnp.concatenate(
            [
                jnp.where(here, b, 0).astype(jnp.float32).astype(jnp.bfloat16),
                jnp.where(here, lane, 0).astype(jnp.float32).astype(jnp.bfloat16),
            ],
            axis=0,
        )
        right = jnp.where(lo_line == (atoms & (BLK - 1)), 1.0, 0.0).astype(jnp.bfloat16)
        found = found + lax.dot_general(left, right, (((1,), (1,)), ((), ())), preferred_element_type=jnp.float32)
    inverse_out[...] = (found[:blocks] * BLK + found[blocks:]).astype(jnp.int32)

    slot_lane = lax.broadcasted_iota(jnp.int32, (blocks, slots), 1)
    slot_line = lax.broadcasted_iota(jnp.int32, (blocks, slots), 0)
    listed = (own_lanes[...] == slot_line) & (slot_lane < pair_count[...])
    table[...] = jnp.where(listed, 1.0, 0.0).astype(jnp.bfloat16)

    for copy in moved_meta:
        copy.wait_recv()

    def choose(read):
        here = read(0)
        own_flag, col_flag = (jnp.broadcast_to(meta[k, 2:3, :], here.shape) for k in (0, 2))
        taken = jnp.broadcast_to(accept_col[...], here.shape)
        mine = jnp.where(own_flag == 1.0, read(1), here)
        theirs = jnp.where(col_flag == 1.0, read(3), read(2))
        return jnp.where(taken == 1, theirs, mine)

    def choose_all(buffer, target):
        chosen[...] = choose(lambda k: buffer[k])
        for c in range(3):
            target[:, c * BLK:(c + 1) * BLK] = permuted(
                lambda s: chosen[c * blocks + s:c * blocks + s + 1, :], blocks, order
            )

    centre = choose(lambda k: meta[k])

    for copy in moved_x:
        copy.wait_recv()
    choose_all(raw_x, x_ref)

    def halo(t):
        mine = near.at[t, pl.ds(rows_slab, rows_slab), :]
        down = pltpu.make_async_remote_copy(
            src_ref=mine,
            dst_ref=near.at[t, pl.ds(2 * rows_slab, rows_slab), :],
            send_sem=halo_send.at[t, 0],
            recv_sem=halo_recv.at[t, 0],
            device_id={"dom": lax.max(dom - 1, 0)},
            device_id_type=MESH,
        )
        up = pltpu.make_async_remote_copy(
            src_ref=mine,
            dst_ref=near.at[t, pl.ds(0, rows_slab), :],
            send_sem=halo_send.at[t, 1],
            recv_sem=halo_recv.at[t, 1],
            device_id={"dom": lax.min(dom + 1, domains - 1)},
            device_id_type=MESH,
        )
        return down, up

    def shares(t):
        return [
            pltpu.make_async_remote_copy(
                src_ref=partial.at[t, 0],
                dst_ref=partial.at[t, k + 1],
                send_sem=cv_send.at[t, k],
                recv_sem=cv_recv.at[t, k],
                device_id=peers[k],
                device_id_type=MESH,
            )
            for k in range(domains - 1)
        ]

    has_lower = dom > 0
    has_upper = dom < domains - 1

    def evaluate(t, carry):
        @pl.when(t > 0)
        def _():
            speeds = v_ref[...] + (0.5 * DT) * mass[...] * f_ref[...]
            v_ref[...] = speeds
            x_ref[...] = x_ref[...] + DT * speeds
        now = x_ref[...]
        scaled = [KAPPA * now[:, c * BLK:(c + 1) * BLK] for c in range(3)]
        norm = -0.5 * (scaled[0] * scaled[0] + scaled[1] * scaled[1] + scaled[2] * scaled[2])
        for c, rows in enumerate(scaled + [norm]):
            near[t, pl.ds(rows_slab + c, blocks, stride=4), :] = rows
        down, up = halo(t)
        pl.when(has_lower)(down.start)
        pl.when(has_upper)(up.start)
        for k in range(2):
            product = weights[k] * now
            folded = product[:8] + product[8:]
            folded = folded[:, :BLK] + folded[:, BLK:2 * BLK] + folded[:, 2 * BLK:]
            partial[t, 0, k:k + 1, :] = jnp.sum(folded, axis=0, keepdims=True)
        sent = shares(t)
        for copy in sent:
            copy.start()
        @pl.when(t == 0)
        def _():
            for copy in moved_v:
                copy.wait_recv()
            choose_all(raw_v, v_ref)

        def block_rows(b):
            four = near[t, 4 * b:4 * b + 4, :]
            return jnp.concatenate([four, four], axis=0)

        for b in range(blocks):
            rows = block_rows(blocks + b)
            partners_tab[blocks + b] = partner_rows(jnp.where(line == 7, 1.0, rows), line)
            owners_tab[b] = owner_rows(
                jnp.where(line == 3, 1.0, jnp.where(line == 7, rows + LOG2_EPS, rows)), line
            )
        pl.when(has_lower)(up.wait_recv)
        pl.when(has_upper)(down.wait_recv)
        for b in list(range(blocks)) + list(range(2 * blocks, 3 * blocks)):
            partners_tab[b] = partner_rows(jnp.where(line == 7, 1.0, block_rows(b)), line)

        def add_tiles(group, carry):
            for u in range(UNROLL):
                first = group * (2 * UNROLL) + 2 * u
                sums = two_tiles(
                    partners_tab,
                    owners_tab,
                    [pair_other[0, first + k] for k in range(2)],
                    [pair_own[0, first + k] for k in range(2)],
                )
                for k in range(2):
                    tiles[pl.ds(pl.multiple_of(16 * (first + k), 16), 16), :] = sums[k]
            return carry

        lax.fori_loop(0, slots // (2 * UNROLL), add_tiles, 0)

        def slot_rows(r):
            return tiles[pl.ds(r, slots, stride=16), :]

        listed_rows = jnp.concatenate(
            [slot_rows(c) + slot_rows(8 + c) + slot_rows(12 + c) for c in range(3)] + [slot_rows(7)], axis=1
        )
        pair = jnp.zeros((blocks, 4 * BLK), jnp.float32)
        for piece in split3(listed_rows):
            pair = pair + jnp.dot(table[...], piece, preferred_element_type=jnp.float32)
        total = pair[:, 3 * BLK:]
        force = now * jnp.concatenate([total, total, total], axis=1) - (1.0 / KAPPA) * pair[:, :3 * BLK]
        for copy in sent:
            copy.wait_recv()
        share = partial[t, 0]
        for k in range(1, domains):
            share = share + partial[t, k]
        for k in range(2):
            value = jnp.sum(share[k:k + 1], axis=1, keepdims=True)
            force = force - (stiffness[0:1, k:k + 1] * (value - centre[k:k + 1, 0:1])) * weights[k]
        f_ref[...] = force
        @pl.when(t > 0)
        def _():
            v_ref[...] = v_ref[...] + (0.5 * DT) * mass[...] * force

        return carry

    lax.fori_loop(0, EVALS, evaluate, 0)

    state_out[0:blocks, :] = x_ref[...]
    state_out[blocks:2 * blocks, :] = v_ref[...]
    state_out[2 * blocks:3 * blocks, :] = f_ref[...]

    for copy in moved_meta + moved_x + moved_v:
        copy.wait_send()
    for t in range(EVALS):
        down, up = halo(t)
        pl.when(has_lower)(down.wait_send)
        pl.when(has_upper)(up.wait_send)
        for copy in shares(t):
            copy.wait_send()


def restore(state, inverse, x_out, v_out, f_out):
    blocks = inverse.shape[0]
    index = inverse[...]
    for a, out in enumerate((x_out, v_out, f_out)):
        for c in range(3):
            value = permuted(
                lambda s: state[a * blocks + s:a * blocks + s + 1, c * BLK:(c + 1) * BLK], blocks, index
            )
            out[c * blocks:(c + 1) * blocks, :] = value


def per_device(
    domains,
    positions,
    velocities,
    inv_mass,
    cv_weight,
    stiffness,
    centers,
    block_order,
    pair_count,
    pair_own,
    pair_other,
    accept_row,
    accept_col,
):
    atoms = block_order.shape[0]
    blocks = atoms // BLK
    slots = pair_own.shape[1]
    f32 = jnp.float32
    vmem = pl.BlockSpec(memory_space=VMEM)
    anywhere = pl.BlockSpec(memory_space=pltpu.HBM)
    dma = pltpu.SemaphoreType.DMA
    wide = 3 * BLK
    state, inverse = pl.pallas_call(
        functools.partial(simulate, domains, slots),
        out_shape=(
            jax.ShapeDtypeStruct((3 * blocks, wide), f32),
            jax.ShapeDtypeStruct((blocks, BLK), jnp.int32),
        ),
        in_specs=[anywhere] * 13,
        out_specs=(vmem, vmem),
        scratch_shapes=[
            VMEM((blocks, BLK), f32),
            VMEM((6 * blocks, BLK), f32),
            VMEM((blocks, BLK), jnp.int32),
            VMEM((1, slots), jnp.int32),
            VMEM((1, 2), f32),
            VMEM((1, 2), f32),
            VMEM((1, 1), jnp.int32),
            VMEM((1, 1), jnp.int32),
            VMEM((1, 1), jnp.int32),
            SMEM((1, slots), jnp.int32),
            SMEM((1, slots), jnp.int32),
            VMEM((4, 3 * blocks, BLK), f32),
            VMEM((4, 3 * blocks, BLK), f32),
            VMEM((4, 8, BLK), f32),
            VMEM((3 * blocks, BLK), f32),
            VMEM((blocks, wide), f32),
            VMEM((blocks, wide), f32),
            VMEM((blocks, wide), f32),
            VMEM((EVALS, 12 * blocks, BLK), f32),
            VMEM((2, blocks, wide), f32),
            VMEM((blocks, wide), f32),
            VMEM((blocks, slots), jnp.bfloat16),
            VMEM((16 * slots, BLK), f32),
            VMEM((3 * blocks, 32, BLK), jnp.bfloat16),
            VMEM((blocks, 32, BLK), jnp.bfloat16),
            VMEM((EVALS, domains, 2, BLK), f32),
            dma((13,)),
            dma((3, 3)),
            dma((3, 3)),
            dma((EVALS, 2)),
            dma((EVALS, 2)),
            dma((EVALS, domains - 1)),
            dma((EVALS, domains - 1)),
        ],
        compiler_params=pltpu.CompilerParams(collective_id=0, has_side_effects=True),
        name="simulate",
    )(
        positions.reshape(3 * blocks, BLK),
        velocities.reshape(3 * blocks, BLK),
        inv_mass.reshape(blocks, BLK),
        cv_weight.reshape(2, 3, blocks, BLK).transpose(1, 2, 0, 3).reshape(6 * blocks, BLK),
        block_order.reshape(blocks, BLK),
        pair_own,
        stiffness[None],
        centers[0],
        pair_count[None],
        accept_row,
        accept_col,
        pair_own,
        pair_other,
    )
    outs = pl.pallas_call(
        restore,
        out_shape=(jax.ShapeDtypeStruct((3 * blocks, BLK), f32),) * 3,
        in_specs=[vmem] * 2,
        out_specs=(vmem,) * 3,
        name="restore",
    )(state, inverse)
    return tuple(out.reshape(1, 1, 3, atoms) for out in outs)


def solution(mesh):
    placed = (
        P("wrow", "wcol", None, "dom"),
        P("wrow", "wcol", None, "dom"),
        P("dom"),
        P(None, None, "dom"),
        P(),
        P("wrow", "wcol", None),
        P("dom"),
        P("dom"),
        P("dom", None),
        P("dom", None),
        P("wrow", "wcol"),
        P("wrow", "wcol"),
    )
    return jax.shard_map(
        functools.partial(per_device, mesh.shape["dom"]),
        mesh=mesh,
        in_specs=placed,
        out_specs=(P("wrow", "wcol", None, "dom"),) * 3,
        check_vma=False,
    )
```

```python
import functools
import math

import jax
import jax.numpy as jnp
from jax import lax
from jax.experimental import pallas as pl
from jax.experimental.pallas import tpu as pltpu
from jax.sharding import PartitionSpec as P

BLK = 128
STEPS = 3
EVALS = STEPS + 1
UNROLL = 32
LOG2_EPS = -6.0
DT = 0.1
KAPPA = math.sqrt(math.log2(math.e))
MESH = pl.DeviceIdType.MESH
VMEM = pltpu.VMEM
SMEM = pltpu.SMEM


def lane_take(rows, lanes):
    dims = lax.GatherDimensionNumbers(
        offset_dims=(),
        collapsed_slice_dims=(1,),
        start_index_map=(1,),
        operand_batching_dims=(0,),
        start_indices_batching_dims=(0,),
    )
    return lax.gather(
        rows, lanes[..., None], dims, slice_sizes=(1, 1), mode=lax.GatherScatterMode.PROMISE_IN_BOUNDS
    )


def permuted(source_row, blocks, index):
    halves = []
    for half in range(blocks // 8):
        piece = index[half * 8:(half + 1) * 8]
        lanes = piece & (BLK - 1)
        owner = piece >> 7
        total = jnp.zeros((8, BLK), jnp.float32)
        for s in range(blocks):
            taken = lane_take(jnp.broadcast_to(source_row(s), (8, BLK)), lanes)
            total = jnp.where(owner == s, taken, total)
        halves.append(total)
    return jnp.concatenate(halves, axis=0)


def split3(value):
    high = value.astype(jnp.bfloat16)
    rest = value - high.astype(jnp.float32)
    mid = rest.astype(jnp.bfloat16)
    low = (rest - mid.astype(jnp.float32)).astype(jnp.bfloat16)
    return high, mid, low


def split2(value):
    high = value.astype(jnp.bfloat16)
    return high, (value - high.astype(jnp.float32)).astype(jnp.bfloat16)


def stack_groups(groups):
    zero = jnp.zeros((8, BLK), jnp.float32)
    upper = jnp.concatenate(groups[:2], axis=0).astype(jnp.bfloat16)
    lower = jnp.concatenate([groups[2], zero], axis=0).astype(jnp.bfloat16)
    return jnp.concatenate([upper, lower], axis=0)


def parts(value):
    return [piece.astype(jnp.float32) for piece in split3(value)]


def partner_rows(rows, line):
    high, mid, low = parts(rows)
    middle = (line > 3) & (line < 7)
    return stack_groups(
        [
            high,
            jnp.where(line < 4, mid, jnp.where(line == 7, high, low)),
            jnp.where(line == 3, low, jnp.where(middle, mid, high)),
        ]
    )


def owner_rows(rows, line):
    high, mid, low = parts(rows)
    middle = (line > 3) & (line < 7)
    return stack_groups(
        [
            jnp.where(middle, mid, high),
            jnp.where(line == 7, mid, high),
            jnp.where(line == 3, high, jnp.where(middle, mid, low)),
        ]
    )


def two_tiles(partners, owners, other, own):
    left = [partners[q] for q in other]
    right = [owners[b] for b in own]
    zero = jnp.zeros_like(right[0])
    power = lax.dot_general(
        jnp.concatenate(left, axis=0),
        jnp.concatenate(
            [jnp.concatenate([right[0], zero], axis=1), jnp.concatenate([zero, right[1]], axis=1)], axis=0
        ),
        (((0,), (0,)), ((), ())),
        preferred_element_type=jnp.float32,
    )
    weight = jnp.concatenate(split2(jnp.exp2(jnp.minimum(power, LOG2_EPS))), axis=0)
    heads = [jnp.concatenate([rows[:16], rows[:16]], axis=1) for rows in left]
    sums = jnp.dot(jnp.concatenate(heads, axis=0), weight, preferred_element_type=jnp.float32)
    return sums[:16, :BLK], sums[16:, BLK:]


def simulate(domains, slots, *refs):
    inputs, refs = refs[:13], refs[13:]
    (state_out, inverse_out), refs = refs[:2], refs[2:]
    local, refs = refs[:11], refs[11:]
    inv_mass, cv_weight, block_order, own_lanes, stiffness, centers, pair_count = local[:7]
    accept_row, accept_col, pair_own, pair_other = local[7:]
    raw_x, raw_v, meta, chosen, x_ref, v_ref, f_ref, near = refs[:8]
    weights, mass, table, tiles, partners_tab, owners_tab, partial = refs[8:15]
    in_sem, swap_send, swap_recv, halo_send, halo_recv, cv_send, cv_recv = refs[15:]
    row = lax.axis_index("wrow")
    col = lax.axis_index("wcol")
    dom = lax.axis_index("dom")
    blocks = block_order.shape[0]
    rows_slab = 4 * blocks
    partners = [
        {"wrow": row ^ 1},
        {"wcol": col ^ 1},
        {"wrow": row ^ 1, "wcol": col ^ 1},
    ]
    peers = [{"dom": lax.rem(dom + k, domains)} for k in range(1, domains)]

    barrier = pltpu.get_barrier_semaphore()
    for device in partners + peers:
        pl.semaphore_signal(barrier, inc=1, device_id=device, device_id_type=MESH)
    arrivals = [
        pltpu.make_async_copy(source, target, in_sem.at[k])
        for k, (source, target) in enumerate(zip(inputs, (raw_x.at[0], raw_v.at[0]) + local))
    ]
    for k in (0, 7, 9, 1, 4, 2, 3, 5, 6, 8, 10, 11, 12):
        arrivals[k].start()
    own_x, own_v = arrivals[:2]
    arrivals[7].wait()
    arrivals[9].wait()

    line = lax.broadcasted_iota(jnp.int32, (8, BLK), 0)
    meta[0] = jnp.where(
        line == 0, centers[0:1, 0:1], jnp.where(line == 1, centers[0:1, 1:2], accept_row[...].astype(jnp.float32))
    )

    own_x.wait()
    pl.semaphore_wait(barrier, len(partners) + len(peers))

    def swap(buffer, which):
        return [
            pltpu.make_async_remote_copy(
                src_ref=buffer.at[0],
                dst_ref=buffer.at[k + 1],
                send_sem=swap_send.at[which, k],
                recv_sem=swap_recv.at[which, k],
                device_id=partners[k],
                device_id_type=MESH,
            )
            for k in (2, 0, 1)
        ]

    moved_x, moved_v, moved_meta = swap(raw_x, 0), swap(raw_v, 1), swap(meta, 2)
    for copy in moved_meta:
        copy.start()
    for copy in moved_x:
        copy.start()
    own_v.wait()
    for copy in moved_v:
        copy.start()

    for k in (4, 2, 3, 5, 6, 8, 10, 11, 12):
        arrivals[k].wait()
    order = block_order[...]
    for k in range(2):
        for c in range(3):
            weights[k, :, c * BLK:(c + 1) * BLK] = permuted(
                lambda s: cv_weight[(c * blocks + s) * 2 + k:(c * blocks + s) * 2 + k + 1, :], blocks, order
            )
    mass_now = permuted(lambda s: inv_mass[s:s + 1, :], blocks, order)
    for c in range(3):
        mass[:, c * BLK:(c + 1) * BLK] = mass_now

    lane = lax.broadcasted_iota(jnp.int32, (blocks, BLK), 1)
    hi_line = lax.broadcasted_iota(jnp.int32, (blocks, BLK), 0)
    lo_line = lax.broadcasted_iota(jnp.int32, (BLK, BLK), 0)
    found = jnp.zeros((2 * blocks, BLK), jnp.float32)
    for b in range(blocks):
        atoms = order[b:b + 1]
        here = hi_line == (atoms >> 7)
        left = jnp.concatenate(
            [
                jnp.where(here, b, 0).astype(jnp.float32).astype(jnp.bfloat16),
                jnp.where(here, lane, 0).astype(jnp.float32).astype(jnp.bfloat16),
            ],
            axis=0,
        )
        right = jnp.where(lo_line == (atoms & (BLK - 1)), 1.0, 0.0).astype(jnp.bfloat16)
        found = found + lax.dot_general(left, right, (((1,), (1,)), ((), ())), preferred_element_type=jnp.float32)
    inverse_out[...] = (found[:blocks] * BLK + found[blocks:]).astype(jnp.int32)

    slot_lane = lax.broadcasted_iota(jnp.int32, (blocks, slots), 1)
    slot_line = lax.broadcasted_iota(jnp.int32, (blocks, slots), 0)
    listed = (own_lanes[...] == slot_line) & (slot_lane < pair_count[...])
    table[...] = jnp.where(listed, 1.0, 0.0).astype(jnp.bfloat16)

    for copy in moved_meta:
        copy.wait_recv()

    def choose(read):
        here = read(0)
        own_flag, col_flag = (jnp.broadcast_to(meta[k, 2:3, :], here.shape) for k in (0, 2))
        taken = jnp.broadcast_to(accept_col[...], here.shape)
        mine = jnp.where(own_flag == 1.0, read(1), here)
        theirs = jnp.where(col_flag == 1.0, read(3), read(2))
        return jnp.where(taken == 1, theirs, mine)

    def choose_all(buffer, target):
        chosen[...] = choose(lambda k: buffer[k])
        for c in range(3):
            target[:, c * BLK:(c + 1) * BLK] = permuted(
                lambda s: chosen[c * blocks + s:c * blocks + s + 1, :], blocks, order
            )

    centre = choose(lambda k: meta[k])

    for copy in moved_x:
        copy.wait_recv()
    choose_all(raw_x, x_ref)

    def halo(t):
        mine = near.at[t, pl.ds(rows_slab, rows_slab), :]
        down = pltpu.make_async_remote_copy(
            src_ref=mine,
            dst_ref=near.at[t, pl.ds(2 * rows_slab, rows_slab), :],
            send_sem=halo_send.at[t, 0],
            recv_sem=halo_recv.at[t, 0],
            device_id={"dom": lax.max(dom - 1, 0)},
            device_id_type=MESH,
        )
        up = pltpu.make_async_remote_copy(
            src_ref=mine,
            dst_ref=near.at[t, pl.ds(0, rows_slab), :],
            send_sem=halo_send.at[t, 1],
            recv_sem=halo_recv.at[t, 1],
            device_id={"dom": lax.min(dom + 1, domains - 1)},
            device_id_type=MESH,
        )
        return down, up

    def shares(t):
        return [
            pltpu.make_async_remote_copy(
                src_ref=partial.at[t, 0],
                dst_ref=partial.at[t, k + 1],
                send_sem=cv_send.at[t, k],
                recv_sem=cv_recv.at[t, k],
                device_id=peers[k],
                device_id_type=MESH,
            )
            for k in range(domains - 1)
        ]

    has_lower = dom > 0
    has_upper = dom < domains - 1

    def evaluate(t, carry):
        @pl.when(t > 0)
        def _():
            speeds = v_ref[...] + (0.5 * DT) * mass[...] * f_ref[...]
            v_ref[...] = speeds
            x_ref[...] = x_ref[...] + DT * speeds
        now = x_ref[...]
        scaled = [KAPPA * now[:, c * BLK:(c + 1) * BLK] for c in range(3)]
        norm = -0.5 * (scaled[0] * scaled[0] + scaled[1] * scaled[1] + scaled[2] * scaled[2])
        for c, rows in enumerate(scaled + [norm]):
            near[t, pl.ds(rows_slab + c, blocks, stride=4), :] = rows
        down, up = halo(t)
        pl.when(has_lower)(down.start)
        pl.when(has_upper)(up.start)
        for k in range(2):
            product = weights[k] * now
            folded = product[:8] + product[8:]
            folded = folded[:, :BLK] + folded[:, BLK:2 * BLK] + folded[:, 2 * BLK:]
            partial[t, 0, k:k + 1, :] = jnp.sum(folded, axis=0, keepdims=True)
        sent = shares(t)
        for copy in sent:
            copy.start()
        @pl.when(t == 0)
        def _():
            for copy in moved_v:
                copy.wait_recv()
            choose_all(raw_v, v_ref)

        def block_rows(b):
            four = near[t, 4 * b:4 * b + 4, :]
            return jnp.concatenate([four, four], axis=0)

        for b in range(blocks):
            rows = block_rows(blocks + b)
            partners_tab[blocks + b] = partner_rows(jnp.where(line == 7, 1.0, rows), line)
            owners_tab[b] = owner_rows(
                jnp.where(line == 3, 1.0, jnp.where(line == 7, rows + LOG2_EPS, rows)), line
            )
        pl.when(has_lower)(up.wait_recv)
        pl.when(has_upper)(down.wait_recv)
        for b in list(range(blocks)) + list(range(2 * blocks, 3 * blocks)):
            partners_tab[b] = partner_rows(jnp.where(line == 7, 1.0, block_rows(b)), line)

        def add_tiles(group, carry):
            for u in range(UNROLL):
                first = group * (2 * UNROLL) + 2 * u
                sums = two_tiles(
                    partners_tab,
                    owners_tab,
                    [pair_other[0, first + k] for k in range(2)],
                    [pair_own[0, first + k] for k in range(2)],
                )
                for k in range(2):
                    tiles[pl.ds(pl.multiple_of(16 * (first + k), 16), 16), :] = sums[k]
            return carry

        lax.fori_loop(0, slots // (2 * UNROLL), add_tiles, 0)

        def slot_rows(r):
            return tiles[pl.ds(r, slots, stride=16), :]

        listed_rows = jnp.concatenate(
            [slot_rows(c) + slot_rows(8 + c) + slot_rows(12 + c) for c in range(3)] + [slot_rows(7)], axis=1
        )
        pair = jnp.zeros((blocks, 4 * BLK), jnp.float32)
        for piece in split3(listed_rows):
            pair = pair + jnp.dot(table[...], piece, preferred_element_type=jnp.float32)
        total = pair[:, 3 * BLK:]
        force = now * jnp.concatenate([total, total, total], axis=1) - (1.0 / KAPPA) * pair[:, :3 * BLK]
        for copy in sent:
            copy.wait_recv()
        share = partial[t, 0]
        for k in range(1, domains):
            share = share + partial[t, k]
        for k in range(2):
            value = jnp.sum(share[k:k + 1], axis=1, keepdims=True)
            force = force - (stiffness[0:1, k:k + 1] * (value - centre[k:k + 1, 0:1])) * weights[k]
        f_ref[...] = force
        @pl.when(t > 0)
        def _():
            v_ref[...] = v_ref[...] + (0.5 * DT) * mass[...] * force

        return carry

    lax.fori_loop(0, EVALS, evaluate, 0)

    state_out[0:blocks, :] = x_ref[...]
    state_out[blocks:2 * blocks, :] = v_ref[...]
    state_out[2 * blocks:3 * blocks, :] = f_ref[...]

    for copy in moved_meta + moved_x + moved_v:
        copy.wait_send()
    for t in range(EVALS):
        down, up = halo(t)
        pl.when(has_lower)(down.wait_send)
        pl.when(has_upper)(up.wait_send)
        for copy in shares(t):
            copy.wait_send()


def restore(state, inverse, x_out, v_out, f_out):
    blocks = inverse.shape[0]
    index = inverse[...]
    for a, out in enumerate((x_out, v_out, f_out)):
        for c in range(3):
            value = permuted(
                lambda s: state[a * blocks + s:a * blocks + s + 1, c * BLK:(c + 1) * BLK], blocks, index
            )
            out[c * blocks:(c + 1) * blocks, :] = value


def hbm(x):
    return x if x.size == 1 else pltpu.with_memory_space_constraint(x, pltpu.HBM)


def per_device(
    domains,
    positions,
    velocities,
    inv_mass,
    cv_weight,
    stiffness,
    centers,
    block_order,
    pair_count,
    pair_own,
    pair_other,
    accept_row,
    accept_col,
):
    atoms = block_order.shape[0]
    blocks = atoms // BLK
    slots = pair_own.shape[1]
    f32 = jnp.float32
    vmem = pl.BlockSpec(memory_space=VMEM)
    anywhere = pl.BlockSpec(memory_space=pltpu.HBM)
    dma = pltpu.SemaphoreType.DMA
    wide = 3 * BLK
    state, inverse = pl.pallas_call(
        functools.partial(simulate, domains, slots),
        out_shape=(
            jax.ShapeDtypeStruct((3 * blocks, wide), f32),
            jax.ShapeDtypeStruct((blocks, BLK), jnp.int32),
        ),
        in_specs=[anywhere] * 13,
        out_specs=(vmem, vmem),
        scratch_shapes=[
            VMEM((blocks, BLK), f32),
            VMEM((6 * blocks, BLK), f32),
            VMEM((blocks, BLK), jnp.int32),
            VMEM((1, slots), jnp.int32),
            VMEM((1, 2), f32),
            VMEM((1, 2), f32),
            VMEM((1, 1), jnp.int32),
            VMEM((1, 1), jnp.int32),
            VMEM((1, 1), jnp.int32),
            SMEM((1, slots), jnp.int32),
            SMEM((1, slots), jnp.int32),
            VMEM((4, 3 * blocks, BLK), f32),
            VMEM((4, 3 * blocks, BLK), f32),
            VMEM((4, 8, BLK), f32),
            VMEM((3 * blocks, BLK), f32),
            VMEM((blocks, wide), f32),
            VMEM((blocks, wide), f32),
            VMEM((blocks, wide), f32),
            VMEM((EVALS, 12 * blocks, BLK), f32),
            VMEM((2, blocks, wide), f32),
            VMEM((blocks, wide), f32),
            VMEM((blocks, slots), jnp.bfloat16),
            VMEM((16 * slots, BLK), f32),
            VMEM((3 * blocks, 32, BLK), jnp.bfloat16),
            VMEM((blocks, 32, BLK), jnp.bfloat16),
            VMEM((EVALS, domains, 2, BLK), f32),
            dma((13,)),
            dma((3, 3)),
            dma((3, 3)),
            dma((EVALS, 2)),
            dma((EVALS, 2)),
            dma((EVALS, domains - 1)),
            dma((EVALS, domains - 1)),
        ],
        compiler_params=pltpu.CompilerParams(collective_id=0, has_side_effects=True, vmem_limit_bytes=16 * 2**20),
        name="simulate",
    )(
        *map(hbm, (
        positions.reshape(3 * blocks, BLK),
        velocities.reshape(3 * blocks, BLK),
        inv_mass.reshape(blocks, BLK),
        cv_weight.reshape(2, 3, blocks, BLK).transpose(1, 2, 0, 3).reshape(6 * blocks, BLK),
        block_order.reshape(blocks, BLK),
        pair_own,
        stiffness[None],
        centers[0],
        pair_count[None],
        accept_row,
        accept_col,
        pair_own,
        pair_other,
        ))
    )
    outs = pl.pallas_call(
        restore,
        out_shape=(jax.ShapeDtypeStruct((3 * blocks, BLK), f32),) * 3,
        in_specs=[vmem] * 2,
        out_specs=(vmem,) * 3,
        compiler_params=pltpu.CompilerParams(vmem_limit_bytes=8 * 2**20),
        name="restore",
    )(state, inverse)
    return tuple(out.reshape(1, 1, 3, atoms) for out in outs)


def solution(mesh):
    placed = (
        P("wrow", "wcol", None, "dom"),
        P("wrow", "wcol", None, "dom"),
        P("dom"),
        P(None, None, "dom"),
        P(),
        P("wrow", "wcol", None),
        P("dom"),
        P("dom"),
        P("dom", None),
        P("dom", None),
        P("wrow", "wcol"),
        P("wrow", "wcol"),
    )
    return jax.shard_map(
        functools.partial(per_device, mesh.shape["dom"]),
        mesh=mesh,
        in_specs=placed,
        out_specs=(P("wrow", "wcol", None, "dom"),) * 3,
        check_vma=False,
    )
```

```python
import functools
import math

import jax
import jax.numpy as jnp
from jax import lax
from jax.experimental import pallas as pl
from jax.experimental.pallas import tpu as pltpu
from jax.sharding import PartitionSpec as P

BLK = 128
STEPS = 3
EVALS = STEPS + 1
UNROLL = 32
LOG2_EPS = -6.0
DT = 0.1
KAPPA = math.sqrt(math.log2(math.e))
MESH = pl.DeviceIdType.MESH
VMEM = pltpu.VMEM
SMEM = pltpu.SMEM


def lane_take(rows, lanes):
    dims = lax.GatherDimensionNumbers(
        offset_dims=(),
        collapsed_slice_dims=(1,),
        start_index_map=(1,),
        operand_batching_dims=(0,),
        start_indices_batching_dims=(0,),
    )
    return lax.gather(
        rows, lanes[..., None], dims, slice_sizes=(1, 1), mode=lax.GatherScatterMode.PROMISE_IN_BOUNDS
    )


def permuted(source_row, blocks, index):
    halves = []
    for half in range(blocks // 8):
        piece = index[half * 8:(half + 1) * 8]
        lanes = piece & (BLK - 1)
        owner = piece >> 7
        total = jnp.zeros((8, BLK), jnp.float32)
        for s in range(blocks):
            taken = lane_take(jnp.broadcast_to(source_row(s), (8, BLK)), lanes)
            total = jnp.where(owner == s, taken, total)
        halves.append(total)
    return jnp.concatenate(halves, axis=0)


def split3(value):
    high = value.astype(jnp.bfloat16)
    rest = value - high.astype(jnp.float32)
    mid = rest.astype(jnp.bfloat16)
    low = (rest - mid.astype(jnp.float32)).astype(jnp.bfloat16)
    return high, mid, low


def split2(value):
    high = value.astype(jnp.bfloat16)
    return high, (value - high.astype(jnp.float32)).astype(jnp.bfloat16)


def stack_groups(groups):
    zero = jnp.zeros((8, BLK), jnp.float32)
    upper = jnp.concatenate(groups[:2], axis=0).astype(jnp.bfloat16)
    lower = jnp.concatenate([groups[2], zero], axis=0).astype(jnp.bfloat16)
    return jnp.concatenate([upper, lower], axis=0)


def parts(value):
    return [piece.astype(jnp.float32) for piece in split3(value)]


def partner_rows(rows, line):
    high, mid, low = parts(rows)
    middle = (line > 3) & (line < 7)
    return stack_groups(
        [
            high,
            jnp.where(line < 4, mid, jnp.where(line == 7, high, low)),
            jnp.where(line == 3, low, jnp.where(middle, mid, high)),
        ]
    )


def owner_rows(rows, line):
    high, mid, low = parts(rows)
    middle = (line > 3) & (line < 7)
    return stack_groups(
        [
            jnp.where(middle, mid, high),
            jnp.where(line == 7, mid, high),
            jnp.where(line == 3, high, jnp.where(middle, mid, low)),
        ]
    )


def two_tiles(partners, owners, other, own):
    left = [partners[q] for q in other]
    right = [owners[b] for b in own]
    zero = jnp.zeros_like(right[0])
    power = lax.dot_general(
        jnp.concatenate(left, axis=0),
        jnp.concatenate(
            [jnp.concatenate([right[0], zero], axis=1), jnp.concatenate([zero, right[1]], axis=1)], axis=0
        ),
        (((0,), (0,)), ((), ())),
        preferred_element_type=jnp.float32,
    )
    weight = jnp.concatenate(split2(jnp.exp2(jnp.minimum(power, LOG2_EPS))), axis=0)
    heads = [jnp.concatenate([rows[:16], rows[:16]], axis=1) for rows in left]
    sums = jnp.dot(jnp.concatenate(heads, axis=0), weight, preferred_element_type=jnp.float32)
    return sums[:16, :BLK], sums[16:, BLK:]


def simulate(domains, slots, *refs):
    inputs, refs = refs[:12], refs[12:]
    (state_out, inverse_out), refs = refs[:2], refs[2:]
    local, refs = refs[:11], refs[11:]
    inv_mass, cv_weight, block_order, own_lanes, other_lanes, stiffness, centers = local[:7]
    pair_count, accept_row, accept_col, named = local[7:]
    home_x, home_v, raw_x, raw_v, meta, fresh, x_ref, v_ref, f_ref, near = refs[:10]
    weights, mass, lists, table, tiles, partners_tab, owners_tab, partial = refs[10:18]
    in_sem, list_sem, swap_send, swap_recv, twin_send, twin_recv = refs[18:24]
    halo_send, halo_recv, cv_send, cv_recv = refs[24:]
    row = lax.axis_index("wrow")
    col = lax.axis_index("wcol")
    dom = lax.axis_index("dom")
    blocks = block_order.shape[0]
    rows_slab = 4 * blocks
    last = EVALS - 1

    def place(d):
        return d ^ (d >> 1)

    spot = place(dom)
    moved = spot != dom
    role = jnp.where(moved, 1, 0)
    twin = {"dom": spot}
    partners = [
        {"wrow": row ^ 1, "dom": spot},
        {"wcol": col ^ 1, "dom": spot},
        {"wrow": row ^ 1, "wcol": col ^ 1, "dom": spot},
    ]
    peers = [{"dom": lax.rem(dom + k, domains)} for k in range(1, domains)]

    barrier = pltpu.get_barrier_semaphore()
    for device in partners + peers:
        pl.semaphore_signal(barrier, inc=1, device_id=device, device_id_type=MESH)
    arrivals = [
        pltpu.make_async_copy(source, target, in_sem.at[k])
        for k, (source, target) in enumerate(zip(inputs, (fresh.at[0], fresh.at[1]) + local[:10]))
    ]
    for k in (4, 0, 8, 10, 1, 2, 3, 5, 6, 7, 9, 11):
        arrivals[k].start()
    own_x, own_v = arrivals[:2]
    arrivals[8].wait()
    arrivals[10].wait()

    line = lax.broadcasted_iota(jnp.int32, (8, BLK), 0)
    meta[0] = jnp.where(
        line == 0, centers[0:1, 0:1], jnp.where(line == 1, centers[0:1, 1:2], accept_row[...].astype(jnp.float32))
    )

    arrivals[4].wait()
    order = block_order[...]

    def reorder(which, target):
        for c in range(3):
            target[c * blocks:(c + 1) * blocks, :] = permuted(
                lambda s: fresh[which, c * blocks + s:c * blocks + s + 1, :], blocks, order
            )

    own_x.wait()
    reorder(0, home_x)

    @pl.when(jnp.logical_not(moved))
    def _():
        raw_x[0] = home_x[...]

    pl.semaphore_wait(barrier, len(partners) + len(peers))

    def swap(source, buffer, which):
        return [
            pltpu.make_async_remote_copy(
                src_ref=source,
                dst_ref=buffer.at[k + 1],
                send_sem=swap_send.at[which, k],
                recv_sem=swap_recv.at[which, k],
                device_id=partners[k],
                device_id_type=MESH,
            )
            for k in (2, 0, 1)
        ]

    def to_twin(source, target, k):
        return pltpu.make_async_remote_copy(
            src_ref=source,
            dst_ref=target,
            send_sem=twin_send.at[k],
            recv_sem=twin_recv.at[k],
            device_id=twin,
            device_id_type=MESH,
        )

    moved_x, moved_v = swap(home_x, raw_x, 0), swap(home_v, raw_v, 1)
    moved_meta = swap(meta.at[0], meta, 2)
    twin_x, twin_v = to_twin(home_x, raw_x.at[0], 0), to_twin(home_v, raw_v.at[0], 1)
    twin_rest = [
        to_twin(weights.at[0], weights.at[1], 2),
        to_twin(mass.at[0], mass.at[1], 3),
        to_twin(lists.at[0], lists.at[1], 4),
    ]
    twin_state = [to_twin(x_ref.at[1], x_ref.at[0], 5), to_twin(v_ref.at[1], v_ref.at[0], 6)]
    for copy in moved_meta:
        copy.start()
    for copy in moved_x:
        copy.start()
    pl.when(moved)(twin_x.start)
    own_v.wait()
    reorder(1, home_v)

    @pl.when(jnp.logical_not(moved))
    def _():
        raw_v[0] = home_v[...]

    for copy in moved_v:
        copy.start()
    pl.when(moved)(twin_v.start)

    for k in (2, 3, 5, 6, 7, 9, 11):
        arrivals[k].wait()
    for k in range(2):
        for c in range(3):
            weights[0, k, :, c * BLK:(c + 1) * BLK] = permuted(
                lambda s: cv_weight[(c * blocks + s) * 2 + k:(c * blocks + s) * 2 + k + 1, :], blocks, order
            )
    mass_now = permuted(lambda s: inv_mass[s:s + 1, :], blocks, order)
    for c in range(3):
        mass[0, :, c * BLK:(c + 1) * BLK] = mass_now
    gap = jnp.zeros((1, BLK - slots), jnp.int32)
    listing = [jnp.concatenate([rows[...], gap], axis=1) for rows in (own_lanes, other_lanes)]
    lists[0] = jnp.where(line == 0, listing[0], jnp.where(line == 1, listing[1], pair_count[...]))

    @pl.when(moved)
    def _():
        for copy in twin_rest:
            copy.start()


    lane = lax.broadcasted_iota(jnp.int32, (blocks, BLK), 1)
    hi_line = lax.broadcasted_iota(jnp.int32, (blocks, BLK), 0)
    lo_line = lax.broadcasted_iota(jnp.int32, (BLK, BLK), 0)
    found = jnp.zeros((2 * blocks, BLK), jnp.float32)
    for b in range(blocks):
        atoms = order[b:b + 1]
        here = hi_line == (atoms >> 7)
        left = jnp.concatenate(
            [
                jnp.where(here, b, 0).astype(jnp.float32).astype(jnp.bfloat16),
                jnp.where(here, lane, 0).astype(jnp.float32).astype(jnp.bfloat16),
            ],
            axis=0,
        )
        right = jnp.where(lo_line == (atoms & (BLK - 1)), 1.0, 0.0).astype(jnp.bfloat16)
        found = found + lax.dot_general(left, right, (((1,), (1,)), ((), ())), preferred_element_type=jnp.float32)
    inverse_out[...] = (found[:blocks] * BLK + found[blocks:]).astype(jnp.int32)

    def use_lists(which):
        slot_lane = lax.broadcasted_iota(jnp.int32, (blocks, slots), 1)
        slot_line = lax.broadcasted_iota(jnp.int32, (blocks, slots), 0)
        listed = (lists[which, 0:1, :slots] == slot_line) & (slot_lane < lists[which, 2:3, :slots])
        table[which] = jnp.where(listed, 1.0, 0.0).astype(jnp.bfloat16)
        copy = pltpu.make_async_copy(lists.at[which], named.at[which], list_sem.at[which])
        copy.start()
        copy.wait()

    use_lists(0)

    for copy in moved_meta:
        copy.wait_recv()

    def choose(read):
        here = read(0)
        own_flag, col_flag = (jnp.broadcast_to(meta[k, 2:3, :], here.shape) for k in (0, 2))
        taken = jnp.broadcast_to(accept_col[...], here.shape)
        mine = jnp.where(own_flag == 1.0, read(1), here)
        theirs = jnp.where(col_flag == 1.0, read(3), read(2))
        return jnp.where(taken == 1, theirs, mine)

    def choose_all(buffer, target):
        picked = choose(lambda k: buffer[k])
        for c in range(3):
            target[role, :, c * BLK:(c + 1) * BLK] = picked[c * blocks:(c + 1) * blocks]

    centre = choose(lambda k: meta[k])

    for copy in moved_x:
        copy.wait_recv()
    pl.when(moved)(twin_x.wait_recv)
    choose_all(raw_x, x_ref)

    @pl.when(moved)
    def _():
        for copy in twin_rest:
            copy.wait_recv()
        use_lists(1)


    def frame(t):
        return jnp.where(t == last, dom, spot)

    def mine_at(t):
        return pl.multiple_of((spot - frame(t) + 1) * rows_slab, rows_slab)

    def halo(t):
        sides = []
        for side in range(3):
            target = spot - (side - 1)
            device = jnp.where(t == last, target, place(jnp.clip(target, 0, domains - 1)))
            device = jnp.clip(device, 0, domains - 1)
            inside = (target >= 0) & (target < domains)
            copy = pltpu.make_async_remote_copy(
                src_ref=near.at[t, pl.ds(mine_at(t), rows_slab), :],
                dst_ref=near.at[t, pl.ds(side * rows_slab, rows_slab), :],
                send_sem=halo_send.at[t, side],
                recv_sem=halo_recv.at[t, side],
                device_id={"dom": device},
                device_id_type=MESH,
            )
            wanted = frame(t) + (side - 1)
            held = (wanted >= 0) & (wanted < domains)
            sides.append((copy, inside & (device != dom), held & (wanted != spot)))
        return sides

    def shares(t):
        return [
            pltpu.make_async_remote_copy(
                src_ref=partial.at[t, 0],
                dst_ref=partial.at[t, k + 1],
                send_sem=cv_send.at[t, k],
                recv_sem=cv_recv.at[t, k],
                device_id=peers[k],
                device_id_type=MESH,
            )
            for k in range(domains - 1)
        ]

    def evaluate(t, carry):
        @pl.when(t > 0)
        def _():
            speeds = v_ref[role] + (0.5 * DT) * mass[role] * f_ref[...]
            v_ref[role] = speeds
            x_ref[role] = x_ref[role] + DT * speeds
        here = x_ref[role]
        scaled = [KAPPA * here[:, c * BLK:(c + 1) * BLK] for c in range(3)]
        norm = -0.5 * (scaled[0] * scaled[0] + scaled[1] * scaled[1] + scaled[2] * scaled[2])
        for c, rows in enumerate(scaled + [norm]):
            near[t, pl.ds(mine_at(t) + c, blocks, stride=4), :] = rows
        sides = halo(t)
        for side in (0, 2, 1):
            pl.when(sides[side][1])(sides[side][0].start)
        closing = (t == last) & moved

        @pl.when(closing)
        def _():
            for copy in twin_state:
                copy.start()

        for k in range(2):
            product = weights[role, k] * here
            folded = product[:8] + product[8:]
            folded = folded[:, :BLK] + folded[:, BLK:2 * BLK] + folded[:, 2 * BLK:]
            partial[t, 0, k:k + 1, :] = jnp.sum(folded, axis=0, keepdims=True)
        sent = shares(t)
        for copy in sent:
            copy.start()
        @pl.when(t == 0)
        def _():
            for copy in moved_v:
                copy.wait_recv()
            pl.when(moved)(twin_v.wait_recv)
            choose_all(raw_v, v_ref)

        pl.when(sides[1][2])(sides[1][0].wait_recv)
        for b in range(blocks):
            four = near[t, 4 * (blocks + b):4 * (blocks + b) + 4, :]
            rows = jnp.concatenate([four, four], axis=0)
            partners_tab[blocks + b] = partner_rows(jnp.where(line == 7, 1.0, rows), line)
            owners_tab[b] = owner_rows(
                jnp.where(line == 3, 1.0, jnp.where(line == 7, rows + LOG2_EPS, rows)), line
            )

        def build(first):
            for b in range(blocks):
                four = near[t, pl.ds(pl.multiple_of(4 * (first + b), 4), 4), :]
                rows = jnp.concatenate([four, four], axis=0)
                partners_tab[first + b] = partner_rows(jnp.where(line == 7, 1.0, rows), line)

        parity = lax.rem(frame(t), 2)
        odd = parity == 1
        even = jnp.logical_not(odd)
        lower, upper = sides[0], sides[2]
        pl.when(lower[2] & odd)(lower[0].wait_recv)
        pl.when(upper[2] & even)(upper[0].wait_recv)
        build(2 * blocks * (1 - parity))
        pl.when(lower[2] & even)(lower[0].wait_recv)
        pl.when(upper[2] & odd)(upper[0].wait_recv)
        build(2 * blocks * parity)
        held = jnp.where(t == last, 0, role)

        @pl.when(closing)
        def _():
            for copy in twin_state:
                copy.wait_recv()

        now = x_ref[held]

        def add_tiles(group, carry):
            for u in range(UNROLL):
                first = group * (2 * UNROLL) + 2 * u
                sums = two_tiles(
                    partners_tab,
                    owners_tab,
                    [named[held, 1, first + k] for k in range(2)],
                    [named[held, 0, first + k] for k in range(2)],
                )
                for k in range(2):
                    tiles[pl.ds(pl.multiple_of(16 * (first + k), 16), 16), :] = sums[k]
            return carry

        lax.fori_loop(0, slots // (2 * UNROLL), add_tiles, 0)

        def slot_rows(r):
            return tiles[pl.ds(r, slots, stride=16), :]

        listed_rows = jnp.concatenate(
            [slot_rows(c) + slot_rows(8 + c) + slot_rows(12 + c) for c in range(3)] + [slot_rows(7)], axis=1
        )
        pair = jnp.zeros((blocks, 4 * BLK), jnp.float32)
        for piece in split3(listed_rows):
            pair = pair + jnp.dot(table[held], piece, preferred_element_type=jnp.float32)
        total = pair[:, 3 * BLK:]
        force = now * jnp.concatenate([total, total, total], axis=1) - (1.0 / KAPPA) * pair[:, :3 * BLK]
        for copy in sent:
            copy.wait_recv()
        share = partial[t, 0]
        for k in range(1, domains):
            share = share + partial[t, k]
        for k in range(2):
            value = jnp.sum(share[k:k + 1], axis=1, keepdims=True)
            force = force - (stiffness[0:1, k:k + 1] * (value - centre[k:k + 1, 0:1])) * weights[held, k]
        f_ref[...] = force
        @pl.when(t > 0)
        def _():
            v_ref[held] = v_ref[held] + (0.5 * DT) * mass[held] * force

        return carry

    lax.fori_loop(0, EVALS, evaluate, 0)

    state_out[0:blocks, :] = x_ref[0]
    state_out[blocks:2 * blocks, :] = v_ref[0]
    state_out[2 * blocks:3 * blocks, :] = f_ref[...]

    for copy in moved_meta + moved_x + moved_v:
        copy.wait_send()

    @pl.when(moved)
    def _():
        for copy in [twin_x, twin_v] + twin_rest + twin_state:
            copy.wait_send()

    for t in range(EVALS):
        for copy, sent_now, _ in halo(t):
            pl.when(sent_now)(copy.wait_send)
        for copy in shares(t):
            copy.wait_send()


def restore(state, inverse, x_out, v_out, f_out):
    blocks = inverse.shape[0]
    index = inverse[...]
    for a, out in enumerate((x_out, v_out, f_out)):
        for c in range(3):
            value = permuted(
                lambda s: state[a * blocks + s:a * blocks + s + 1, c * BLK:(c + 1) * BLK], blocks, index
            )
            out[c * blocks:(c + 1) * blocks, :] = value


def hbm(x):
    return x if x.size == 1 else pltpu.with_memory_space_constraint(x, pltpu.HBM)


def per_device(
    domains,
    positions,
    velocities,
    inv_mass,
    cv_weight,
    stiffness,
    centers,
    block_order,
    pair_count,
    pair_own,
    pair_other,
    accept_row,
    accept_col,
):
    atoms = block_order.shape[0]
    blocks = atoms // BLK
    slots = pair_own.shape[1]
    f32 = jnp.float32
    vmem = pl.BlockSpec(memory_space=VMEM)
    anywhere = pl.BlockSpec(memory_space=pltpu.HBM)
    dma = pltpu.SemaphoreType.DMA
    wide = 3 * BLK
    state, inverse = pl.pallas_call(
        functools.partial(simulate, domains, slots),
        out_shape=(
            jax.ShapeDtypeStruct((3 * blocks, wide), f32),
            jax.ShapeDtypeStruct((blocks, BLK), jnp.int32),
        ),
        in_specs=[anywhere] * 12,
        out_specs=(vmem, vmem),
        scratch_shapes=[
            VMEM((blocks, BLK), f32),
            VMEM((6 * blocks, BLK), f32),
            VMEM((blocks, BLK), jnp.int32),
            VMEM((1, slots), jnp.int32),
            VMEM((1, slots), jnp.int32),
            VMEM((1, 2), f32),
            VMEM((1, 2), f32),
            VMEM((1, 1), jnp.int32),
            VMEM((1, 1), jnp.int32),
            VMEM((1, 1), jnp.int32),
            SMEM((2, 8, BLK), jnp.int32),
            VMEM((3 * blocks, BLK), f32),
            VMEM((3 * blocks, BLK), f32),
            VMEM((4, 3 * blocks, BLK), f32),
            VMEM((4, 3 * blocks, BLK), f32),
            VMEM((4, 8, BLK), f32),
            VMEM((2, 3 * blocks, BLK), f32),
            VMEM((2, blocks, wide), f32),
            VMEM((2, blocks, wide), f32),
            VMEM((blocks, wide), f32),
            VMEM((EVALS, 12 * blocks, BLK), f32),
            VMEM((2, 2, blocks, wide), f32),
            VMEM((2, blocks, wide), f32),
            VMEM((2, 8, BLK), jnp.int32),
            VMEM((2, blocks, slots), jnp.bfloat16),
            VMEM((16 * slots, BLK), f32),
            VMEM((3 * blocks, 32, BLK), jnp.bfloat16),
            VMEM((blocks, 32, BLK), jnp.bfloat16),
            VMEM((EVALS, domains, 2, BLK), f32),
            dma((12,)),
            dma((2,)),
            dma((3, 3)),
            dma((3, 3)),
            dma((7,)),
            dma((7,)),
            dma((EVALS, 3)),
            dma((EVALS, 3)),
            dma((EVALS, domains - 1)),
            dma((EVALS, domains - 1)),
        ],
        compiler_params=pltpu.CompilerParams(collective_id=0, has_side_effects=True, vmem_limit_bytes=16 * 2**20),
        name="simulate",
    )(
        *map(hbm, (
        positions.reshape(3 * blocks, BLK),
        velocities.reshape(3 * blocks, BLK),
        inv_mass.reshape(blocks, BLK),
        cv_weight.reshape(2, 3, blocks, BLK).transpose(1, 2, 0, 3).reshape(6 * blocks, BLK),
        block_order.reshape(blocks, BLK),
        pair_own,
        pair_other,
        stiffness[None],
        centers[0],
        pair_count[None],
        accept_row,
        accept_col,
        ))
    )
    outs = pl.pallas_call(
        restore,
        out_shape=(jax.ShapeDtypeStruct((3 * blocks, BLK), f32),) * 3,
        in_specs=[vmem] * 2,
        out_specs=(vmem,) * 3,
        compiler_params=pltpu.CompilerParams(vmem_limit_bytes=8 * 2**20),
        name="restore",
    )(state, inverse)
    return tuple(out.reshape(1, 1, 3, atoms) for out in outs)


def solution(mesh):
    placed = (
        P("wrow", "wcol", None, "dom"),
        P("wrow", "wcol", None, "dom"),
        P("dom"),
        P(None, None, "dom"),
        P(),
        P("wrow", "wcol", None),
        P("dom"),
        P("dom"),
        P("dom", None),
        P("dom", None),
        P("wrow", "wcol"),
        P("wrow", "wcol"),
    )
    return jax.shard_map(
        functools.partial(per_device, mesh.shape["dom"]),
        mesh=mesh,
        in_specs=placed,
        out_specs=(P("wrow", "wcol", None, "dom"),) * 3,
        check_vma=False,
    )
```

```python
import functools
import math

import jax
import jax.numpy as jnp
from jax import lax
from jax.experimental import pallas as pl
from jax.experimental.pallas import tpu as pltpu
from jax.sharding import PartitionSpec as P

BLK = 128
STEPS = 3
EVALS = STEPS + 1
UNROLL = 32
LOG2_EPS = -6.0
DT = 0.1
KAPPA = math.sqrt(math.log2(math.e))
MESH = pl.DeviceIdType.MESH
VMEM = pltpu.VMEM
SMEM = pltpu.SMEM


def lane_take(rows, lanes):
    dims = lax.GatherDimensionNumbers(
        offset_dims=(),
        collapsed_slice_dims=(1,),
        start_index_map=(1,),
        operand_batching_dims=(0,),
        start_indices_batching_dims=(0,),
    )
    return lax.gather(
        rows, lanes[..., None], dims, slice_sizes=(1, 1), mode=lax.GatherScatterMode.PROMISE_IN_BOUNDS
    )


def permuted(source_row, blocks, index):
    halves = []
    for half in range(blocks // 8):
        piece = index[half * 8:(half + 1) * 8]
        lanes = piece & (BLK - 1)
        owner = piece >> 7
        total = jnp.zeros((8, BLK), jnp.float32)
        for s in range(blocks):
            taken = lane_take(jnp.broadcast_to(source_row(s), (8, BLK)), lanes)
            total = jnp.where(owner == s, taken, total)
        halves.append(total)
    return jnp.concatenate(halves, axis=0)


def split3(value):
    high = value.astype(jnp.bfloat16)
    rest = value - high.astype(jnp.float32)
    mid = rest.astype(jnp.bfloat16)
    low = (rest - mid.astype(jnp.float32)).astype(jnp.bfloat16)
    return high, mid, low


def split2(value):
    high = value.astype(jnp.bfloat16)
    return high, (value - high.astype(jnp.float32)).astype(jnp.bfloat16)


def stack_groups(groups):
    zero = jnp.zeros((8, BLK), jnp.float32)
    upper = jnp.concatenate(groups[:2], axis=0).astype(jnp.bfloat16)
    lower = jnp.concatenate([groups[2], zero], axis=0).astype(jnp.bfloat16)
    return jnp.concatenate([upper, lower], axis=0)


def parts(value):
    return [piece.astype(jnp.float32) for piece in split3(value)]


def partner_rows(rows, line):
    high, mid, low = parts(rows)
    middle = (line > 3) & (line < 7)
    return stack_groups(
        [
            high,
            jnp.where(line < 4, mid, jnp.where(line == 7, high, low)),
            jnp.where(line == 3, low, jnp.where(middle, mid, high)),
        ]
    )


def owner_rows(rows, line):
    high, mid, low = parts(rows)
    middle = (line > 3) & (line < 7)
    return stack_groups(
        [
            jnp.where(middle, mid, high),
            jnp.where(line == 7, mid, high),
            jnp.where(line == 3, high, jnp.where(middle, mid, low)),
        ]
    )


def two_tiles(partners, owners, other, own):
    left = [partners[q] for q in other]
    right = [owners[b] for b in own]
    zero = jnp.zeros_like(right[0])
    power = lax.dot_general(
        jnp.concatenate(left, axis=0),
        jnp.concatenate(
            [jnp.concatenate([right[0], zero], axis=1), jnp.concatenate([zero, right[1]], axis=1)], axis=0
        ),
        (((0,), (0,)), ((), ())),
        preferred_element_type=jnp.float32,
    )
    weight = jnp.concatenate(split2(jnp.exp2(jnp.minimum(power, LOG2_EPS))), axis=0)
    heads = [jnp.concatenate([rows[:16], rows[:16]], axis=1) for rows in left]
    sums = jnp.dot(jnp.concatenate(heads, axis=0), weight, preferred_element_type=jnp.float32)
    return sums[:16, :BLK], sums[16:, BLK:]


def simulate(domains, slots, *refs):
    inputs, refs = refs[:12], refs[12:]
    (state_out, inverse_out), refs = refs[:2], refs[2:]
    local, refs = refs[:11], refs[11:]
    inv_mass, cv_weight, block_order, own_lanes, other_lanes, stiffness, centers = local[:7]
    pair_count, accept_row, accept_col, named = local[7:]
    home_x, home_v, raw_x, raw_v, meta, fresh, x_ref, v_ref, f_ref, near = refs[:10]
    weights, mass, lists, table, tiles, partners_tab, owners_tab, partial = refs[10:18]
    in_sem, list_sem, swap_send, swap_recv, twin_send, twin_recv = refs[18:24]
    halo_send, halo_recv, cv_send, cv_recv = refs[24:]
    row = lax.axis_index("wrow")
    col = lax.axis_index("wcol")
    dom = lax.axis_index("dom")
    blocks = block_order.shape[0]
    rows_slab = 4 * blocks
    last = EVALS - 1

    def place(d):
        return d ^ (d >> 1)

    spot = place(dom)
    moved = spot != dom
    role = jnp.where(moved, 1, 0)
    twin = {"dom": spot}
    partners = [
        {"wrow": row ^ 1, "dom": spot},
        {"wcol": col ^ 1, "dom": spot},
        {"wrow": row ^ 1, "wcol": col ^ 1, "dom": spot},
    ]
    peers = [{"dom": lax.rem(dom + k, domains)} for k in range(1, domains)]

    barrier = pltpu.get_barrier_semaphore()
    for device in partners + peers:
        pl.semaphore_signal(barrier, inc=1, device_id=device, device_id_type=MESH)
    arrivals = [
        pltpu.make_async_copy(source, target, in_sem.at[k])
        for k, (source, target) in enumerate(zip(inputs, (fresh.at[0], fresh.at[1]) + local[:10]))
    ]
    for k in (4, 0, 8, 10, 1, 2, 3, 5, 6, 7, 9, 11):
        arrivals[k].start()
    own_x, own_v = arrivals[:2]
    arrivals[8].wait()
    arrivals[10].wait()

    line = lax.broadcasted_iota(jnp.int32, (8, BLK), 0)
    meta[0] = jnp.where(
        line == 0, centers[0:1, 0:1], jnp.where(line == 1, centers[0:1, 1:2], accept_row[...].astype(jnp.float32))
    )

    arrivals[4].wait()
    order = block_order[...]

    def reorder(which, target):
        for c in range(3):
            target[c * blocks:(c + 1) * blocks, :] = permuted(
                lambda s: fresh[which, c * blocks + s:c * blocks + s + 1, :], blocks, order
            )

    own_x.wait()
    reorder(0, home_x)

    @pl.when(jnp.logical_not(moved))
    def _():
        raw_x[0] = home_x[...]

    pl.semaphore_wait(barrier, len(partners) + len(peers))

    def swap(source, buffer, which):
        return [
            pltpu.make_async_remote_copy(
                src_ref=source,
                dst_ref=buffer.at[k + 1],
                send_sem=swap_send.at[which, k],
                recv_sem=swap_recv.at[which, k],
                device_id=partners[k],
                device_id_type=MESH,
            )
            for k in (2, 0, 1)
        ]

    def to_twin(source, target, k):
        return pltpu.make_async_remote_copy(
            src_ref=source,
            dst_ref=target,
            send_sem=twin_send.at[k],
            recv_sem=twin_recv.at[k],
            device_id=twin,
            device_id_type=MESH,
        )

    moved_x, moved_v = swap(home_x, raw_x, 0), swap(home_v, raw_v, 1)
    moved_meta = swap(meta.at[0], meta, 2)
    twin_x, twin_v = to_twin(home_x, raw_x.at[0], 0), to_twin(home_v, raw_v.at[0], 1)
    twin_rest = [
        to_twin(weights.at[0], weights.at[1], 2),
        to_twin(mass.at[0], mass.at[1], 3),
        to_twin(lists.at[0], lists.at[1], 4),
    ]
    twin_state = [to_twin(x_ref.at[1], x_ref.at[0], 5), to_twin(v_ref.at[1], v_ref.at[0], 6)]
    for copy in moved_meta:
        copy.start()
    for copy in moved_x:
        copy.start()
    pl.when(moved)(twin_x.start)
    own_v.wait()
    reorder(1, home_v)

    @pl.when(jnp.logical_not(moved))
    def _():
        raw_v[0] = home_v[...]

    for copy in moved_v:
        copy.start()
    pl.when(moved)(twin_v.start)

    for k in (2, 3, 5, 6, 7, 9, 11):
        arrivals[k].wait()
    for k in range(2):
        for c in range(3):
            weights[0, k, :, c * BLK:(c + 1) * BLK] = permuted(
                lambda s: cv_weight[(c * blocks + s) * 2 + k:(c * blocks + s) * 2 + k + 1, :], blocks, order
            )
    mass_now = permuted(lambda s: inv_mass[s:s + 1, :], blocks, order)
    for c in range(3):
        mass[0, :, c * BLK:(c + 1) * BLK] = mass_now
    gap = jnp.zeros((1, BLK - slots), jnp.int32)
    listing = [jnp.concatenate([rows[...], gap], axis=1) for rows in (own_lanes, other_lanes)]
    lists[0] = jnp.where(line == 0, listing[0], jnp.where(line == 1, listing[1], pair_count[...]))

    @pl.when(moved)
    def _():
        for copy in twin_rest:
            copy.start()


    lane = lax.broadcasted_iota(jnp.int32, (blocks, BLK), 1)
    hi_line = lax.broadcasted_iota(jnp.int32, (blocks, BLK), 0)
    lo_line = lax.broadcasted_iota(jnp.int32, (BLK, BLK), 0)
    found = jnp.zeros((2 * blocks, BLK), jnp.float32)
    for b in range(blocks):
        atoms = order[b:b + 1]
        here = hi_line == (atoms >> 7)
        left = jnp.concatenate(
            [
                jnp.where(here, b, 0).astype(jnp.float32).astype(jnp.bfloat16),
                jnp.where(here, lane, 0).astype(jnp.float32).astype(jnp.bfloat16),
            ],
            axis=0,
        )
        right = jnp.where(lo_line == (atoms & (BLK - 1)), 1.0, 0.0).astype(jnp.bfloat16)
        found = found + lax.dot_general(left, right, (((1,), (1,)), ((), ())), preferred_element_type=jnp.float32)
    inverse_out[...] = (found[:blocks] * BLK + found[blocks:]).astype(jnp.int32)

    def use_lists(which):
        slot_lane = lax.broadcasted_iota(jnp.int32, (blocks, slots), 1)
        slot_line = lax.broadcasted_iota(jnp.int32, (blocks, slots), 0)
        listed = (lists[which, 0:1, :slots] == slot_line) & (slot_lane < lists[which, 2:3, :slots])
        table[which] = jnp.where(listed, 1.0, 0.0).astype(jnp.bfloat16)
        copy = pltpu.make_async_copy(lists.at[which], named.at[which], list_sem.at[which])
        copy.start()
        copy.wait()

    use_lists(0)

    for copy in moved_meta:
        copy.wait_recv()

    def choose(read):
        here = read(0)
        own_flag, col_flag = (jnp.broadcast_to(meta[k, 2:3, :], here.shape) for k in (0, 2))
        taken = jnp.broadcast_to(accept_col[...], here.shape)
        mine = jnp.where(own_flag == 1.0, read(1), here)
        theirs = jnp.where(col_flag == 1.0, read(3), read(2))
        return jnp.where(taken == 1, theirs, mine)

    def choose_all(buffer, target):
        picked = choose(lambda k: buffer[k])
        for c in range(3):
            target[role, :, c * BLK:(c + 1) * BLK] = picked[c * blocks:(c + 1) * blocks]

    centre = choose(lambda k: meta[k])

    for copy in moved_x:
        copy.wait_recv()
    pl.when(moved)(twin_x.wait_recv)
    choose_all(raw_x, x_ref)

    @pl.when(moved)
    def _():
        for copy in twin_rest:
            copy.wait_recv()
        use_lists(1)


    def frame(t):
        return jnp.where(t == last, dom, spot)

    def mine_at(t):
        return pl.multiple_of((spot - frame(t) + 1) * rows_slab, rows_slab)

    def halo(t):
        sides = []
        for side in range(3):
            target = spot - (side - 1)
            device = jnp.where(t == last, target, place(jnp.clip(target, 0, domains - 1)))
            device = jnp.clip(device, 0, domains - 1)
            inside = (target >= 0) & (target < domains)
            copy = pltpu.make_async_remote_copy(
                src_ref=near.at[t, pl.ds(mine_at(t), rows_slab), :],
                dst_ref=near.at[t, pl.ds(side * rows_slab, rows_slab), :],
                send_sem=halo_send.at[t, side],
                recv_sem=halo_recv.at[t, side],
                device_id={"dom": device},
                device_id_type=MESH,
            )
            wanted = frame(t) + (side - 1)
            held = (wanted >= 0) & (wanted < domains)
            sides.append((copy, inside & (device != dom), held & (wanted != spot)))
        return sides

    def shares(t):
        return [
            pltpu.make_async_remote_copy(
                src_ref=partial.at[t, 0],
                dst_ref=partial.at[t, k + 1],
                send_sem=cv_send.at[t, k],
                recv_sem=cv_recv.at[t, k],
                device_id=peers[k],
                device_id_type=MESH,
            )
            for k in range(domains - 1)
        ]

    def evaluate(t, carry):
        @pl.when(t > 0)
        def _():
            speeds = v_ref[role] + (0.5 * DT) * mass[role] * f_ref[...]
            v_ref[role] = speeds
            x_ref[role] = x_ref[role] + DT * speeds
        here = x_ref[role]
        scaled = [KAPPA * here[:, c * BLK:(c + 1) * BLK] for c in range(3)]
        norm = -0.5 * (scaled[0] * scaled[0] + scaled[1] * scaled[1] + scaled[2] * scaled[2])
        for c, rows in enumerate(scaled + [norm]):
            near[t, pl.ds(mine_at(t) + c, blocks, stride=4), :] = rows
        sides = halo(t)
        for side in (0, 2, 1):
            pl.when(sides[side][1])(sides[side][0].start)
        closing = (t == last) & moved

        @pl.when(closing)
        def _():
            for copy in twin_state:
                copy.start()

        for k in range(2):
            product = weights[role, k] * here
            folded = product[:8] + product[8:]
            folded = folded[:, :BLK] + folded[:, BLK:2 * BLK] + folded[:, 2 * BLK:]
            partial[t, 0, k:k + 1, :] = jnp.sum(folded, axis=0, keepdims=True)
        sent = shares(t)
        for copy in sent:
            copy.start()
        @pl.when(t == 0)
        def _():
            for copy in moved_v:
                copy.wait_recv()
            pl.when(moved)(twin_v.wait_recv)
            choose_all(raw_v, v_ref)

        pl.when(sides[1][2])(sides[1][0].wait_recv)
        for b in range(blocks):
            four = near[t, 4 * (blocks + b):4 * (blocks + b) + 4, :]
            rows = jnp.concatenate([four, four], axis=0)
            partners_tab[blocks + b] = partner_rows(jnp.where(line == 7, 1.0, rows), line)
            owners_tab[b] = owner_rows(
                jnp.where(line == 3, 1.0, jnp.where(line == 7, rows + LOG2_EPS, rows)), line
            )

        def build(first):
            for b in range(blocks):
                four = near[t, pl.ds(pl.multiple_of(4 * (first + b), 4), 4), :]
                rows = jnp.concatenate([four, four], axis=0)
                partners_tab[first + b] = partner_rows(jnp.where(line == 7, 1.0, rows), line)

        parity = lax.rem(frame(t), 2)
        odd = parity == 1
        even = jnp.logical_not(odd)
        lower, upper = sides[0], sides[2]
        pl.when(lower[2] & odd)(lower[0].wait_recv)
        pl.when(upper[2] & even)(upper[0].wait_recv)
        build(2 * blocks * (1 - parity))
        pl.when(lower[2] & even)(lower[0].wait_recv)
        pl.when(upper[2] & odd)(upper[0].wait_recv)
        build(2 * blocks * parity)
        held = jnp.where(t == last, 0, role)

        @pl.when(closing)
        def _():
            for copy in twin_state:
                copy.wait_recv()

        now = x_ref[held]

        def add_tiles(group, carry):
            for u in range(UNROLL):
                first = group * (2 * UNROLL) + 2 * u
                sums = two_tiles(
                    partners_tab,
                    owners_tab,
                    [named[held, 1, first + k] for k in range(2)],
                    [named[held, 0, first + k] for k in range(2)],
                )
                for k in range(2):
                    tiles[pl.ds(pl.multiple_of(16 * (first + k), 16), 16), :] = sums[k]
            return carry

        lax.fori_loop(0, slots // (2 * UNROLL), add_tiles, 0)

        def slot_rows(r):
            return tiles[pl.ds(r, slots, stride=16), :]

        listed_rows = jnp.concatenate(
            [slot_rows(c) + slot_rows(8 + c) + slot_rows(12 + c) for c in range(3)] + [slot_rows(7)], axis=1
        )
        pair = jnp.zeros((blocks, 4 * BLK), jnp.float32)
        for piece in split3(listed_rows):
            pair = pair + jnp.dot(table[held], piece, preferred_element_type=jnp.float32)
        total = pair[:, 3 * BLK:]
        force = now * jnp.concatenate([total, total, total], axis=1) - (1.0 / KAPPA) * pair[:, :3 * BLK]
        for copy in sent:
            copy.wait_recv()
        share = partial[t, 0]
        for k in range(1, domains):
            share = share + partial[t, k]
        for k in range(2):
            value = jnp.sum(share[k:k + 1], axis=1, keepdims=True)
            force = force - (stiffness[0:1, k:k + 1] * (value - centre[k:k + 1, 0:1])) * weights[held, k]
        f_ref[...] = force
        @pl.when(t > 0)
        def _():
            v_ref[held] = v_ref[held] + (0.5 * DT) * mass[held] * force

        return carry

    lax.fori_loop(0, EVALS, evaluate, 0)

    state_out[0:blocks, :] = x_ref[0]
    state_out[blocks:2 * blocks, :] = v_ref[0]
    state_out[2 * blocks:3 * blocks, :] = f_ref[...]

    for copy in moved_meta + moved_x + moved_v:
        copy.wait_send()

    @pl.when(moved)
    def _():
        for copy in [twin_x, twin_v] + twin_rest + twin_state:
            copy.wait_send()

    for t in range(EVALS):
        for copy, sent_now, _ in halo(t):
            pl.when(sent_now)(copy.wait_send)
        for copy in shares(t):
            copy.wait_send()


def restore(state, inverse, x_out, v_out, f_out):
    blocks = inverse.shape[0]
    index = inverse[...]
    for a, out in enumerate((x_out, v_out, f_out)):
        for c in range(3):
            value = permuted(
                lambda s: state[a * blocks + s:a * blocks + s + 1, c * BLK:(c + 1) * BLK], blocks, index
            )
            out[c * blocks:(c + 1) * blocks, :] = value


def hbm(x):
    return x if x.size == 1 else pltpu.with_memory_space_constraint(x, pltpu.HBM)


def per_device(
    domains,
    positions,
    velocities,
    inv_mass,
    cv_weight,
    stiffness,
    centers,
    block_order,
    pair_count,
    pair_own,
    pair_other,
    accept_row,
    accept_col,
):
    atoms = block_order.shape[0]
    blocks = atoms // BLK
    slots = pair_own.shape[1]
    f32 = jnp.float32
    vmem = pl.BlockSpec(memory_space=VMEM)
    anywhere = pl.BlockSpec(memory_space=pltpu.HBM)
    dma = pltpu.SemaphoreType.DMA
    wide = 3 * BLK
    state, inverse = pl.pallas_call(
        functools.partial(simulate, domains, slots),
        out_shape=(
            jax.ShapeDtypeStruct((3 * blocks, wide), f32),
            jax.ShapeDtypeStruct((blocks, BLK), jnp.int32),
        ),
        in_specs=[anywhere] * 12,
        out_specs=(vmem, vmem),
        scratch_shapes=[
            VMEM((blocks, BLK), f32),
            VMEM((6 * blocks, BLK), f32),
            VMEM((blocks, BLK), jnp.int32),
            VMEM((1, slots), jnp.int32),
            VMEM((1, slots), jnp.int32),
            VMEM((1, 2), f32),
            VMEM((1, 2), f32),
            VMEM((1, 1), jnp.int32),
            VMEM((1, 1), jnp.int32),
            VMEM((1, 1), jnp.int32),
            SMEM((2, 8, BLK), jnp.int32),
            VMEM((3 * blocks, BLK), f32),
            VMEM((3 * blocks, BLK), f32),
            VMEM((4, 3 * blocks, BLK), f32),
            VMEM((4, 3 * blocks, BLK), f32),
            VMEM((4, 8, BLK), f32),
            VMEM((2, 3 * blocks, BLK), f32),
            VMEM((2, blocks, wide), f32),
            VMEM((2, blocks, wide), f32),
            VMEM((blocks, wide), f32),
            VMEM((EVALS, 12 * blocks + 8, BLK), f32),
            VMEM((2, 2, blocks, wide), f32),
            VMEM((2, blocks, wide), f32),
            VMEM((2, 8, BLK), jnp.int32),
            VMEM((2, blocks, slots), jnp.bfloat16),
            VMEM((16 * slots + 16, BLK), f32),
            VMEM((3 * blocks, 32, BLK), jnp.bfloat16),
            VMEM((blocks, 32, BLK), jnp.bfloat16),
            VMEM((EVALS, domains, 2, BLK), f32),
            dma((12,)),
            dma((2,)),
            dma((3, 3)),
            dma((3, 3)),
            dma((7,)),
            dma((7,)),
            dma((EVALS, 3)),
            dma((EVALS, 3)),
            dma((EVALS, domains - 1)),
            dma((EVALS, domains - 1)),
        ],
        compiler_params=pltpu.CompilerParams(collective_id=0, has_side_effects=True, vmem_limit_bytes=16 * 2**20),
        name="simulate",
    )(
        *map(hbm, (
        positions.reshape(3 * blocks, BLK),
        velocities.reshape(3 * blocks, BLK),
        inv_mass.reshape(blocks, BLK),
        cv_weight.reshape(2, 3, blocks, BLK).transpose(1, 2, 0, 3).reshape(6 * blocks, BLK),
        block_order.reshape(blocks, BLK),
        pair_own,
        pair_other,
        stiffness[None],
        centers[0],
        pair_count[None],
        accept_row,
        accept_col,
        ))
    )
    outs = pl.pallas_call(
        restore,
        out_shape=(jax.ShapeDtypeStruct((3 * blocks, BLK), f32),) * 3,
        in_specs=[vmem] * 2,
        out_specs=(vmem,) * 3,
        compiler_params=pltpu.CompilerParams(vmem_limit_bytes=8 * 2**20),
        name="restore",
    )(state, inverse)
    return tuple(out.reshape(1, 1, 3, atoms) for out in outs)


def solution(mesh):
    placed = (
        P("wrow", "wcol", None, "dom"),
        P("wrow", "wcol", None, "dom"),
        P("dom"),
        P(None, None, "dom"),
        P(),
        P("wrow", "wcol", None),
        P("dom"),
        P("dom"),
        P("dom", None),
        P("dom", None),
        P("wrow", "wcol"),
        P("wrow", "wcol"),
    )
    return jax.shard_map(
        functools.partial(per_device, mesh.shape["dom"]),
        mesh=mesh,
        in_specs=placed,
        out_specs=(P("wrow", "wcol", None, "dom"),) * 3,
        check_vma=False,
    )
```
